128 devices in a mesh: rep: 1, dp: 128 (over x, y, z, core).
Axes of the slice: x: 4, y: 4, z: 4, core: 2. Of those that a mesh axis runs over, the one named last changes fastest.
Arguments:
- x: bfloat16 [128, 1024, 768], P(('rep', 'dp'))
- dy: bfloat16 [128, 1024, 768], P(('rep', 'dp'))
- w_gate: bfloat16 [2, 768, 6144], replicated
- w_up: bfloat16 [2, 768, 6144], replicated
- w_down: bfloat16 [2, 6144, 768], replicated
- m_w_gate: float32 [2, 768, 6144], P(None, 'dp')
- m_w_up: float32 [2, 768, 6144], P(None, 'dp')
- m_w_down: float32 [2, 6144, 768], P(None, 'dp')
- v_w_gate: float32 [2, 768, 6144], P(None, 'dp')
- v_w_up: float32 [2, 768, 6144], P(None, 'dp')
- v_w_down: float32 [2, 6144, 768], P(None, 'dp')
Outputs:
- output 1: bfloat16 [2, 768, 6144], P('rep')
- output 2: bfloat16 [2, 768, 6144], P('rep')
- output 3: bfloat16 [2, 6144, 768], P('rep')
- output 4: float32 [2, 768, 6144], P('rep', 'dp')
- output 5: float32 [2, 768, 6144], P('rep', 'dp')
- output 6: float32 [2, 6144, 768], P('rep', 'dp')
- output 7: float32 [2, 768, 6144], P('rep', 'dp')
- output 8: float32 [2, 768, 6144], P('rep', 'dp')
- output 9: float32 [2, 6144, 768], P('rep', 'dp')
All inputs are finite; a program needn't handle non-finite values.
Results may differ from the reference program's by a relative error of at most 0.022.
Values are sent between devices in bfloat16 or wider.
A program may use at most 1.5 GiB of HBM per device.

```python
import jax
import jax.numpy as jnp
from jax import lax

SEQUENCES = 128
TOKENS = 1024
D = 768
FF = 6144
LAYERS = 2
NAMES = ("w_gate", "w_up", "w_down")
SHAPES = {"w_gate": (LAYERS, D, FF), "w_up": (LAYERS, D, FF), "w_down": (LAYERS, FF, D)}


def bump(key, n, height):
    away = (jnp.arange(n, dtype=jnp.int32) - jax.random.randint(key, (), 0, n, jnp.int32)) % n
    return jnp.where(away < n // 8, height, 1.0)


def together(key, own, strength):
    shared = jax.random.normal(key, own.shape[1:], jnp.float32)
    return (own + strength * shared) * lax.rsqrt(1 + strength * strength)


def setup_inputs(seed: int = 0, part: int = 0) -> dict:
    kx, kdy, ka, kb, kz, kf, kh, kl, *keys = jax.random.split(jax.random.key(seed), 8 + 3 * len(NAMES))
    kx, kdy, ka, kb = (jax.random.fold_in(k, part) for k in (kx, kdy, ka, kb))
    kw, km, kv = (keys[i::3] for i in range(3))
    shape = (SEQUENCES, TOKENS, D)
    much_x, much_dy = jax.random.uniform(kz, (2,), jnp.float32, 0.0, 1.0)
    loud = 2.0 ** jax.random.uniform(jax.random.fold_in(kz, 1), (), jnp.float32, -1.0, 2.0)
    layers = 2.0 ** jax.random.uniform(kl, (LAYERS, 1, 1), jnp.float32, -1.0, 1.0)
    x = together(ka, jax.random.normal(kx, shape, jnp.float32), much_x) * bump(kf, D, 4.0)
    dy = together(kb, jax.random.normal(kdy, shape, jnp.float32), much_dy)
    drawn = {"x": x.astype(jnp.bfloat16), "dy": (loud * dy * (SEQUENCES * TOKENS) ** -0.5).astype(jnp.bfloat16)}
    for key, name in zip(kw, NAMES, strict=True):
        w = jax.random.normal(key, SHAPES[name], jnp.float32) * SHAPES[name][1] ** -0.5
        drawn[name] = (w * {"w_gate": 1.0, "w_up": bump(kh, FF, 4.0), "w_down": layers}[name]).astype(jnp.bfloat16)
    for key, name in zip(km, NAMES, strict=True):
        drawn[f"m_{name}"] = 0.1 * jax.random.normal(key, SHAPES[name], jnp.float32)
    for key, name in zip(kv, NAMES, strict=True):
        drawn[f"v_{name}"] = jax.random.uniform(key, SHAPES[name], jnp.float32, 0.005, 0.015)
    return drawn


def matmul(a, w):
    return jnp.dot(a, w, preferred_element_type=jnp.float32).astype(jnp.bfloat16)


def normed(h):
    wide = h.astype(jnp.float32)
    scale = lax.rsqrt(jnp.mean(wide**2, -1, keepdims=True) + 1e-6)
    return (wide * scale).astype(jnp.bfloat16)


def layer(h, w):
    a = normed(h)
    gate = jnp.dot(a, w["w_gate"], preferred_element_type=jnp.float32)
    up = jnp.dot(a, w["w_up"], preferred_element_type=jnp.float32)
    return h + matmul((jax.nn.silu(gate) * up).astype(jnp.bfloat16), w["w_down"])


def adamw(w, m, v, g):
    m = 0.9 * m + 0.1 * g
    v = 0.95 * v + 0.05 * g * g
    step = m * lax.rsqrt(v + 1e-8) + 0.1 * w
    return (w - 0.02 * step).astype(jnp.bfloat16), m, v


def clipped(gradients, sum_of_squares, count):
    factor = jnp.minimum(1.0, 0.5 * lax.rsqrt(sum_of_squares / count + 1e-30))
    return [g * factor for g in gradients]


def stack(weights, h):
    return lax.scan(lambda h, w: (layer(h, w), None), h, weights)[0]


def reference(x, dy, w_gate, w_up, w_down, m_w_gate, m_w_up, m_w_down, v_w_gate, v_w_up, v_w_down):
    weights = dict(zip(NAMES, (w_gate, w_up, w_down), strict=True))

    def take(so_far, sequence):
        h, by_y = sequence
        _, back = jax.vjp(lambda w: stack(w, h), weights)
        return jax.tree.map(lambda total, term: total + term.astype(jnp.float32), so_far, back(by_y)[0]), None

    none_yet = {name: jnp.zeros(w.shape, jnp.float32) for name, w in weights.items()}
    by_weights, _ = lax.scan(take, none_yet, (x, dy))
    gradients = [by_weights[name].astype(jnp.bfloat16).astype(jnp.float32) for name in NAMES]
    gradients = clipped(gradients, sum(jnp.sum(g * g) for g in gradients), sum(g.size for g in gradients))
    new = [
        adamw(w.astype(jnp.float32), m, v, g)
        for w, m, v, g in zip((w_gate, w_up, w_down), (m_w_gate, m_w_up, m_w_down), (v_w_gate, v_w_up, v_w_down), gradients, strict=True)
    ]
    return tuple(one[which] for which in range(3) for one in new)
```

```python
import functools

import jax
import jax.numpy as jnp
from jax import lax
from jax.experimental import pallas as pl
from jax.experimental.pallas import tpu as pltpu
from jax.sharding import PartitionSpec as P

F32, BF16 = jnp.float32, jnp.bfloat16
MESH = pl.DeviceIdType.MESH
ALL = slice(None)
VMEM = pl.BlockSpec(memory_space=pltpu.VMEM)
ANY = pl.BlockSpec(memory_space=pl.ANY)
PARAMS = pltpu.CompilerParams
DMA = pltpu.SemaphoreType.DMA
SIGNALS = pltpu.SemaphoreType.REGULAR

RING, CORES, LAYERS = 4, 2, 2
TORUS = (RING, RING, RING)
AXES = range(len(TORUS))
PARTS = len(TORUS)
PAIR = range(2)
GROUP = RING * CORES
PLANE = RING * RING
OWN = 6
ROWS = OWN * GROUP
HALF = 128
LANES = 2 * HALF
T, D, FF = 1024, 768, 6144
NB = 512
N_J = FF // NB
STRIP = 256


def mib(n):
    return n << 20


def begin(copies):
    for c in copies:
        c.start()


def end(copies):
    for c in copies:
        c.wait()


def received(copies):
    for c in copies:
        c.wait_recv()


def sent(copies):
    for c in copies:
        c.wait_send()


def loop(n, first=0):
    def run(body):
        lax.fori_loop(first, n, lambda i, _: body(i), None)

    return run


def slot(i):
    return i % len(PAIR)


def columns(j, n=NB):
    return pl.ds(pl.multiple_of(j * n, n), n)


def lanes(q, n=HALF):
    return pl.ds(q * n, n)


def around(q):
    return q % RING


def place():
    p = lax.axis_index("dp")
    q = p // CORES
    return (q // PLANE, around(q // RING), around(q)), p % CORES


def number(coords, core):
    x, y, z = coords
    return ((x * RING + y) * RING + z) * CORES + core


def device(coords, core):
    return {"dp": number(coords, core)}


def moved(coords, axis, by):
    return tuple(around(q + by) if a == axis else q for a, q in enumerate(coords))


def signal(sem, where):
    pl.semaphore_signal(sem, inc=1, device_id=where, device_id_type=MESH)


def remote(src, dst, send, recv, where):
    return pltpu.make_async_remote_copy(src_ref=src, dst_ref=dst, send_sem=send, recv_sem=recv, device_id=where, device_id_type=MESH)


def group_peers(coords, core):
    x, y, z = coords
    return [((x, y, around(z + dz)), (core + dc) % CORES) for dz in range(RING) for dc in range(CORES) if dz or dc]


def plane_peers(coords, core):
    x, y, z = coords
    return [((around(x + dx), around(y + dy), z), core) for dx in range(RING) for dy in range(RING) if dx or dy]


def enter(coords, core):
    barrier = pltpu.get_barrier_semaphore()
    peers = group_peers(coords, core) + plane_peers(coords, core)
    for where, c in peers:
        signal(barrier, device(where, c))
    pl.semaphore_wait(barrier, len(peers))


GATE, UP, DOWN = range(3)
ORDER = [(1, which, half) for half in PAIR for which in (GATE, UP)]
ORDER += [(layer, DOWN, half) for layer in (1, 0) for half in PAIR]
ORDER += [(0, which, half) for half in PAIR for which in (GATE, UP)]
UNITS = len(ORDER)
UNIT = {what: u for u, what in enumerate(ORDER)}
WIDE1, DOWN1, DOWN0, WIDE0 = UNIT[1, GATE, 0], UNIT[1, DOWN, 0], UNIT[0, DOWN, 0], UNIT[0, GATE, 0]
EACH = UNITS // LAYERS
AHEAD = len(PAIR)
SIDES = ((0, 1), (1, -1))
PASSED, DIRECT = 1, 0
CELL = (ROWS, HALF)


def tile(half):
    return pl.ds(16 * half, 16 + 16 * half)


def pair_of(half):
    return pl.ds(2 * half, 2)


class Ring:
    def __init__(self, k, stage, coords, core, bufs, ss, rs, credit):
        self.axes = axes_left(k, stage)
        self.axis, self.cut = (k + stage) % PARTS, (k - 1) % PARTS
        self.last = self.axis == self.cut
        self.coords, self.core = coords, core
        self.data, self.ra, self.rb = bufs
        self.ss, self.rs, self.credit = ss, rs, credit
        self.i = coords[self.axis]

    def to(self, by):
        return device(moved(self.coords, self.axis, by), self.core)

    def index(self, place, half):
        at = [place if a == self.axis else pair_of(half) if a == self.cut else ALL for a in self.axes]
        return (*at, tile(half) if self.last else ALL, ALL)

    def landing(self, half):
        return (tile(half), ALL) if self.last else ()

    def out(self, half):
        return self.landing(half) or (*(pair_of(half) if a == self.cut else ALL for a in self.axes if a != self.axis), ALL, ALL)

    def firsts(self):
        out = {}
        for side, by in SIDES:
            for which, step, half in ((PASSED, by + by, 1 - side), (DIRECT, by, side)):
                at = self.index(around(self.i + step), half)
                n = len(out)
                out[side, which] = remote(self.data.at[at], self.ra.at[(side, which) + self.landing(half)], self.ss.at[n], self.rs.at[n], self.to(by))
        return out

    def seconds(self):
        out = []
        for side, by in SIDES:
            at, n = self.landing(1 - side), len(SIDES) * len(PAIR) + side
            out.append(remote(self.ra.at[(side, PASSED) + at], self.rb.at[(side,) + at], self.ss.at[n], self.rs.at[n], self.to(by)))
        return out

    def start(self, again):
        @pl.when(again)
        def _():
            for side, _by in SIDES:
                pl.semaphore_wait(self.credit.at[side], 1)

        begin(self.firsts().values())

    def middle(self):
        copies = self.firsts()
        for side, by in SIDES:
            half = 1 - side
            at = (side, PASSED) + self.landing(half)
            copies[side, PASSED].wait_recv()
            here = self.data[self.index(around(self.i + by), half)].astype(F32)
            self.ra[at] = (here + self.ra[at].astype(F32)).astype(BF16)
        begin(self.seconds())

    def finish(self, store, more):
        copies, passed = self.firsts(), self.seconds()
        for side, _by in SIDES:
            copies[side, DIRECT].wait_recv()
            passed[side].wait_recv()
        for half in PAIR:
            here = self.data[self.index(self.i, half)].astype(F32)
            near = self.ra[(half, DIRECT) + self.landing(half)].astype(F32)
            far = self.rb[(1 - half,) + self.landing(half)].astype(F32)
            store(self.out(half), here + near + far)
        sent([*copies.values(), *passed])

        @pl.when(more)
        def _():
            for side, by in SIDES:
                signal(self.credit.at[side], self.to(-by))


def axes_left(k, stage):
    done = [(k + s) % PARTS for s in range(stage)]
    return [a for a in AXES if a not in done]


class Scatter:
    def __init__(self, grads, bufs, sems):
        self.grads = grads
        self.coords, self.core = place()
        self.partner = device(self.coords, 1 - self.core)
        self.d1, self.r0, self.stages, self.blocks, self.squares = bufs
        self.load_sem, self.s_send, self.s_recv, self.ssem, self.rsem, self.credit, self.s_credit = sems

    def load(self, u, k, layer=0):
        src = self.grads[layer].at[u % EACH, k, self.core]
        return pltpu.make_async_copy(src, self.d1.at[slot(u), k], self.load_sem.at[slot(u), k])

    def swap(self, u, k, layer=0):
        s = slot(u)
        src = self.grads[layer].at[u % EACH, k, 1 - self.core]
        return remote(src, self.r0.at[s, k], self.s_send.at[s, k], self.s_recv.at[s, k], self.partner)

    def rings(self, u, stage):
        s = slot(u)
        return [
            Ring(k, stage, self.coords, self.core, [b.at[s] for b in self.stages[stage][k]], self.ssem.at[s, k, stage], self.rsem.at[s, k, stage],
                 self.credit.at[k, stage])
            for k in range(PARTS)
        ]

    def feed(self, u):
        @pl.when(u >= AHEAD)
        def _():
            pl.semaphore_wait(self.s_credit, 1)

        for layer, its in ((1, u < EACH), (0, u >= EACH)):

            @pl.when(its)
            def _(layer=layer):
                for k in range(PARTS):
                    begin([self.swap(u, k, layer), self.load(u, k, layer)])

    def add(self, u):
        for k in range(PARTS):
            self.load(u, k).wait()
            self.swap(u, k).wait_recv()
            d1, r0 = self.d1.at[slot(u), k], self.r0.at[slot(u), k]

            @loop(PLANE)
            def _(n, d1=d1, r0=r0):
                at = (n // RING, around(n))
                d1[at] = (d1[at].astype(F32) + r0[at].astype(F32)).astype(BF16)

        sent([self.swap(u, k) for k in range(PARTS)])

        @pl.when(u + AHEAD < UNITS)
        def _():
            signal(self.s_credit, self.partner)

        for ring in self.rings(u, 0):
            ring.start(u >= AHEAD)

    def at_stages(self, i, step):
        for stage in AXES:
            u = i - stage

            @pl.when((u >= 0) & (u < UNITS))
            def _(u=u, stage=stage):
                step(u, stage)

    def middles(self, i):
        def step(u, stage):
            for ring in self.rings(u, stage):
                ring.middle()

        self.at_stages(i, step)

    def finishes(self, i):
        def step(u, stage):
            rings = self.rings(u, stage)
            for k, ring in enumerate(rings):
                ring.finish(self.into(u, k, ring, stage), u + AHEAD < UNITS)
            if not rings[0].last:
                for ring in self.rings(u, stage + 1):
                    ring.start(u >= AHEAD)

        self.at_stages(i, step)

    def into(self, u, k, ring, stage):
        def store(at, value):
            value = value.astype(BF16)
            if not ring.last:
                self.stages[stage + 1][k][0][(slot(u),) + at] = value
                return
            self.blocks[(u, k) + at] = value
            value = value.astype(F32)
            self.squares[:] += jnp.sum((value * value).reshape(-1, *self.squares.shape), axis=0)

        return store


PACKED = 80


def packed_row(layer, which, k):
    return OWN * ((layer * len(PAIR) + which) * PARTS + k)


def scatter_scratch():
    two = (len(PAIR),)
    out = [pltpu.VMEM((*two, PARTS, *TORUS, *CELL), BF16)] * len(PAIR)
    for stage in AXES:
        for k in range(PARTS):
            left = [len(PAIR) if a == (k - 1) % PARTS else RING for a in axes_left(k, stage + 1)]
            if left:
                out.append(pltpu.VMEM((*two, *(RING for _ in left), *CELL), BF16))
            out.append(pltpu.VMEM((*two, *two, *two, *left, *CELL), BF16))
            out.append(pltpu.VMEM((*two, *two, *left, *CELL), BF16))
    each = (*two, PARTS)
    out += [pltpu.VMEM((UNITS, PARTS, *CELL), BF16), pltpu.VMEM((8, HALF), F32)]
    out += [DMA(each)] * PARTS + [DMA((*each, PARTS, 6))] * len(PAIR) + [SIGNALS((PARTS, PARTS, *two)), SIGNALS]
    out += [pltpu.VMEM((PACKED, LANES), F32), pltpu.VMEM((GROUP, PACKED, LANES), BF16), pltpu.VMEM((GROUP, PACKED, LANES), BF16)]
    out += [pltpu.VMEM((PLANE, *two, 8, HALF), F32)]
    return out + [DMA((GROUP,))] * 4 + [DMA((PLANE,))] * 2


def scatter_of(grads, scratch):
    scratch = iter(scratch)
    d1, r0 = next(scratch), next(scratch)
    stages = []
    data = [d1.at[:, k] for k in range(PARTS)]
    for stage in AXES:
        row, after = [], []
        for k in range(PARTS):
            if axes_left(k, stage + 1):
                after.append(next(scratch))
            row.append((data[k], next(scratch), next(scratch)))
        stages.append(row)
        data = after
    blocks, squares, *rest = scratch
    return Scatter(grads, (d1, r0, stages, blocks, squares), rest[:7]), rest[7:]


def last_swap(sc, out_ref, own_ref, ss_ref, stage, pack, take, sq, t_send, t_recv, q_send, q_recv, q2_send, q2_recv):
    coords, core = sc.coords, sc.core
    x, y, z = coords
    me = CORES * z + core
    first, second = (sq.at[:, i] for i in PAIR)
    peers = list(enumerate(group_peers(coords, core)))
    first[me] = sc.squares[:]
    squares = [remote(first.at[me], first.at[me], q_send.at[n], q_recv.at[n], device(where, c)) for n, (where, c) in peers]
    takes = [remote(pack.at[CORES * where[-1] + c], take.at[me], t_send.at[n], t_recv.at[n], device(where, c)) for n, (where, c) in peers]
    begin(squares)
    stage[:] = jnp.zeros_like(stage)
    for j in range(GROUP):
        for u, (layer, which, half) in enumerate(ORDER):
            for k in range(PARTS):
                if which != DOWN:
                    stage[pl.ds(packed_row(layer, which, k), OWN), lanes(half)] = sc.blocks[u, k].astype(F32)[OWN * j : OWN * j + OWN]
        pack[j] = stage[:].astype(BF16)
    begin(takes)
    for u, (layer, which, half) in enumerate(ORDER):
        for k in range(PARTS):
            if which == DOWN:
                own_ref[layer, :, lanes(half * PARTS + k)] = sc.blocks[u, k].astype(F32)
    take[me] = pack[me]
    received(squares)
    total = sum(first[j] for j in range(GROUP))
    sent(squares)
    mine = RING * x + y
    second[mine] = total
    squares = [
        remote(second.at[mine], second.at[mine], q2_send.at[n], q2_recv.at[n], device(where, c)) for n, (where, c) in enumerate(plane_peers(coords, core))
    ]
    begin(squares)
    end(takes)
    out_ref[:] = take[:]
    end(squares)
    ss_ref[:] = sum(second[j] for j in range(PLANE))


def gather_kernel(rows_ref, down_ref, wide_out, down0_out, down1_out, last_out, take, stage, t_send, t_recv, own_sem, send, recv, c_send, c_recv):
    coords, core = place()
    x, y, z = coords
    me = CORES * z + core
    partner = device(coords, 1 - core)
    enter(coords, core)
    swaps = []
    for n, (where, c) in enumerate(group_peers(coords, core)):
        swaps.append(remote(rows_ref.at[CORES * where[-1] + c], take.at[me], t_send.at[n], t_recv.at[n], device(where, c)))
    begin(swaps)
    take[me] = rows_ref[me]
    here = (*coords, core)
    own = pltpu.make_async_copy(down_ref.at[1, :, lanes(PARTS - 1, LANES)], last_out.at[here], own_sem)
    own.start()
    down0_out[here] = down_ref[0]
    down1_out[here] = down_ref[1, :, pl.ds(0, D - LANES)]

    def piece(which, k, layer, spot):
        at = tuple(ALL if q is None else q for q in spot)
        if which == DOWN:
            if layer and k == PARTS - 1:
                return last_out.at[(*at, core)]
            return (down0_out, down1_out)[layer].at[(*at, core, ALL, lanes(k, LANES))]
        base = (k * GROUP + core * RING) * LANES
        many = RING if spot[-1] is None else 1
        if many == 1:
            base += spot[-1] * LANES
        return wide_out.at[(layer, which, *at[:-1], ALL, pl.ds(pl.multiple_of(base, many * LANES), many * LANES))]

    received(swaps)
    for j in range(GROUP):
        rows = take[j].astype(F32)
        for q in range(len(stage)):
            stage[q, pl.ds(OWN * j, OWN), :] = rows[OWN * q : OWN * q + OWN]
    for layer in PAIR:
        for which in (GATE, UP):
            for k in range(PARTS):
                at = pl.multiple_of((GROUP * k + RING * core + z) * LANES, LANES)
                wide_out[layer, which, x, y, :, pl.ds(at, LANES)] = stage[packed_row(layer, which, k) // OWN].astype(BF16)
    sent(swaps)
    own.wait()

    def spot(k, turn, by):
        out = []
        for a in AXES:
            its = (k - 1 - a) % PARTS
            out.append(None if its < turn else around(coords[a] + by) if its == turn else coords[a])
        return out

    shares = []

    def share(which, k, layer, turn, by, n):
        ref = piece(which, k, layer, spot(k, turn, by))
        shares.append(remote(ref, ref, c_send.at[k, turn, which, n], c_recv.at[k, turn, which, n], partner))
        shares[-1].start()

    everything = [(which, k, side, by) for which in (GATE, UP, DOWN) for k in range(PARTS) for side, by in SIDES]
    for turn in AXES:

        def copy(which, k, by, n, layer, start):
            ref = piece(which, k, layer, spot(k, turn, start))
            sems = send.at[k, turn, which, n], recv.at[k, turn, which, n]
            return remote(ref, ref, *sems, device(moved(coords, (k - 1 - turn) % PARTS, by), core))

        first = [copy(which, k, by, side, side, 0) for which, k, side, by in everything]
        other = [copy(which, k, by, 2 + side, 1 - side, 0) for which, k, side, by in everything]
        far = [copy(which, k, by, 4 + side, side, -by) for which, k, side, by in everything]
        begin(first)
        begin(other)
        if turn == 0:
            for which, k, side, by in everything:
                share(which, k, side, turn, 0, side)
        for n, (which, k, side, by) in enumerate(everything):
            first[n].wait_recv()
            far[n].start()
            share(which, k, side, turn, -by, 2 + side)
        for n, (which, k, side, by) in enumerate(everything):
            other[n].wait_recv()
            share(which, k, 1 - side, turn, -by, 4 + side)
        for n, (which, k, side, by) in enumerate(everything):
            far[n].wait_recv()
            share(which, k, side, turn, 2, 6 + side)
        sent(first + other + far)
    end(shares)


def all_gather(rows, down):
    owners = (*TORUS, CORES, ROWS)
    return pl.pallas_call(
        gather_kernel,
        out_shape=(
            pltpu.VMEM((LAYERS, len(PAIR), RING, RING, ROWS, FF), BF16),
            pltpu.VMEM((*owners, D), BF16),
            pltpu.VMEM((*owners, D - LANES), BF16),
            jax.ShapeDtypeStruct((*owners, LANES), BF16),
        ),
        in_specs=[VMEM] * 2,
        out_specs=(VMEM, VMEM, VMEM, ANY),
        scratch_shapes=[
            pltpu.VMEM(rows.shape, BF16),
            pltpu.VMEM((LAYERS * len(PAIR) * PARTS, ROWS, LANES), F32),
            *[DMA((GROUP,))] * 2,
            DMA,
            *[DMA((PARTS, PARTS, PARTS, 6))] * 2,
            *[DMA((PARTS, PARTS, PARTS, 8))] * 2,
        ],
        compiler_params=PARAMS(collective_id=1, has_side_effects=True, vmem_limit_bytes=mib(4)),
        name="all_gather",
    )(rows, down)


def put_kernel(wide_ref, down0_ref, down1_ref, last_ref, gate_out, up_out, down_out, bounce, sems):
    def into(ref, start, n):
        return ref.at[(1, *(ALL for _ in bounce.shape[:-1]), pl.ds(start, n))]

    pairs = [(wide_ref.at[layer, which], out.at[layer]) for layer in PAIR for which, out in ((GATE, gate_out), (UP, up_out))]
    pairs += [(down0_ref, down_out.at[0]), (down1_ref, into(down_out, 0, D - LANES))]
    pairs += [(last_ref, bounce), (bounce, into(down_out, D - LANES, LANES))]
    *copies, come, go = [pltpu.make_async_copy(src, dst, sems.at[n]) for n, (src, dst) in enumerate(pairs)]
    come.start()
    begin(copies)
    come.wait()
    go.start()
    end(copies)
    go.wait()


def put(wide, down0, down1, last):
    wide_shape = jax.ShapeDtypeStruct((LAYERS, *wide.shape[2:]), BF16)
    return pl.pallas_call(
        put_kernel,
        out_shape=(wide_shape, wide_shape, jax.ShapeDtypeStruct((LAYERS, *down0.shape), BF16)),
        in_specs=[VMEM, VMEM, VMEM, ANY],
        out_specs=(ANY, ANY, ANY),
        scratch_shapes=[pltpu.VMEM(last.shape, BF16), DMA((GROUP,))],
        compiler_params=PARAMS(vmem_limit_bytes=mib(4)),
        name="put",
    )(wide, down0, down1, last)


def nn(a, b):
    return jnp.dot(a, b, preferred_element_type=F32)


def nt(a, b):
    return lax.dot_general(a, b, (((1,), (1,)), ((), ())), preferred_element_type=F32)


def tn(a, b):
    return lax.dot_general(a, b, (((0,), (0,)), ((), ())), preferred_element_type=F32)


def rms(wide):
    return lax.rsqrt(jnp.mean(wide * wide, -1, keepdims=True) + 1e-6)


def sigmoid(g):
    return 0.5 * jnp.tanh(0.5 * g) + 0.5


def strips():
    return [pl.ds(r, STRIP) for r in range(0, T, STRIP)]


def backwards(g, u, d):
    d = d.astype(BF16).astype(F32)
    sig = sigmoid(g)
    silu = g * sig
    return (d * u * (sig + silu * (1 - sig))).astype(BF16), (d * silu).astype(BF16), silu


def forward_kernel(x_ref, wg_ref, wu_ref, wd_ref, g_ref, u_ref, act_ref, h_ref, a0t_ref, a1_ref, a1t_ref,
                   a0, wg, wu, wd, gate, up, act, w_sem, d_sem, g_sem, a_sem):
    def weights(j):
        s = slot(j)
        return [pltpu.make_async_copy(ref.at[0, :, columns(j)], buf.at[s], w_sem.at[n, s]) for n, (ref, buf) in enumerate(((wg_ref, wg), (wu_ref, wu)))]

    def downs(n):
        return [pltpu.make_async_copy(wd_ref.at[0, :, columns(n, LANES)], wd.at[slot(n)], d_sem.at[slot(n)])]

    def stores(j):
        s = slot(j)
        out = [pltpu.make_async_copy(buf.at[s], ref.at[:, columns(j)], g_sem.at[n, s]) for n, (ref, buf) in enumerate(((g_ref, gate), (u_ref, up)))]
        return out + [pltpu.make_async_copy(act.at[:, columns(j)], act_ref.at[:, columns(j)], a_sem.at[s])]

    def norm(from_ref, to_ref, turned_ref):
        @loop(T // STRIP)
        def _(i):
            rows = columns(i, STRIP)
            wide = from_ref[rows, :].astype(F32)
            a = (wide * rms(wide)).astype(BF16)
            to_ref[rows, :] = a
            turned_ref[:, rows] = a.T

    begin(weights(0))
    begin(downs(0))
    norm(x_ref, a0, a0t_ref)

    @loop(N_J)
    def _(j):
        s = slot(j)
        end(weights(j))

        @pl.when(j >= AHEAD)
        def _():
            end(stores(j - AHEAD))

        @pl.when(j + 1 < N_J)
        def _():
            begin(weights(j + 1))

        for rows in strips():
            g = nn(a0[rows, :], wg[s])
            u = nn(a0[rows, :], wu[s])
            gate[s, rows, :] = g
            up[s, rows, :] = u
            act[rows, columns(j)] = (g * sigmoid(g) * u).astype(BF16)
        begin(stores(j))

    @loop(D // LANES)
    def _(n):
        end(downs(n))

        @pl.when(n + 1 < D // LANES)
        def _():
            begin(downs(n + 1))

        for r in range(0, T, NB):
            rows = pl.ds(r, NB)
            y = nn(act[rows, :], wd[slot(n)]).astype(BF16)
            h_ref[rows, columns(n, LANES)] = x_ref[rows, columns(n, LANES)] + y

    norm(h_ref, a1_ref, a1t_ref)
    for j in PAIR:
        end(stores(N_J - AHEAD + j))


def shaped(dtype, *shapes):
    return tuple(jax.ShapeDtypeStruct(s, dtype) for s in shapes)


def slots(dtype, *shapes):
    return [pltpu.VMEM((len(PAIR), *s), dtype) for s in shapes]


def forward(x, *weights):
    two = len(PAIR)
    return pl.pallas_call(
        forward_kernel,
        out_shape=(*shaped(F32, (T, FF), (T, FF)), *shaped(BF16, (T, FF), (T, D), (D, T), (T, D), (D, T))),
        in_specs=[VMEM, ANY, ANY, ANY],
        out_specs=(ANY, ANY, ANY, VMEM, VMEM, VMEM, VMEM),
        scratch_shapes=[
            pltpu.VMEM((T, D), BF16),
            *slots(BF16, (D, NB), (D, NB), (FF, LANES)),
            *slots(F32, (T, NB), (T, NB)),
            pltpu.VMEM((T, FF), BF16),
            DMA((two, two)),
            DMA((two,)),
            DMA((two, two)),
            DMA((two,)),
        ],
        cost_estimate=pl.CostEstimate(flops=6 * T * D * FF, bytes_accessed=mib(100), transcendentals=T * FF),
        compiler_params=PARAMS(vmem_limit_bytes=mib(62)),
        name="forward",
    )(x, *weights)


def both_of(a, b):
    return tuple(enumerate(zip(a, b, strict=True)))


def tiles_of(layer, wide_refs, down_ref, wide_bufs, down_buf, sem):
    def copies(j):
        s = slot(j)
        wide = [pltpu.make_async_copy(ref.at[layer, :, columns(j)], buf.at[s], sem.at[n, s]) for n, (ref, buf) in both_of(wide_refs, wide_bufs)]
        return wide + [pltpu.make_async_copy(down_ref.at[layer, columns(j)], down_buf.at[s], sem.at[DOWN, s])]

    return copies


def wide_outs(grad_ref, first, bufs, sem):
    def copies(j):
        s, q = slot(j), j % EACH
        u = first + len(PAIR) * (j // EACH)
        return [pltpu.make_async_copy(buf.at[s], grad_ref.at[u + n, q // CORES, q % CORES], sem.at[n, s]) for n, buf in enumerate(bufs)]

    return copies


def wide_terms(at_ref, terms, bufs, s):
    for _n, (src, dst) in both_of(terms, bufs):
        w = nn(at_ref[:], src[:]).astype(BF16)
        for z in range(RING):
            dst[s, :, :, z] = w[:, z * HALF : (z + 1) * HALF].reshape(RING, RING, ROWS, HALF)


def down_loop(grad_ref, first, act_hbm, d_ref, act, out, a_sem, d_sem):
    tiles = FF // D

    def comes(t):
        return [pltpu.make_async_copy(act_hbm.at[:, columns(t, D)], act.at[slot(t)], a_sem.at[slot(t)])]

    def goes(t):
        s = slot(t)
        x, y = t // len(PAIR), pair_of(s)
        return [pltpu.make_async_copy(out.at[s, h], grad_ref.at[first + h, :, :, x, y], d_sem.at[h, s]) for h in PAIR]

    begin(comes(0))

    @loop(tiles)
    def _(t):
        s = slot(t)
        end(comes(t))

        @pl.when(t >= AHEAD)
        def _():
            end(goes(t - AHEAD))

        @pl.when(t + 1 < tiles)
        def _():
            begin(comes(t + 1))

        w = tn(act[s], d_ref[:]).astype(BF16).reshape(len(PAIR), RING, CORES, ROWS, D)
        for h in PAIR:
            for k in range(PARTS):
                at = (h * PARTS + k) * HALF
                for c in range(CORES):
                    out[s, h, k, c] = w[:, :, c, :, at : at + HALF]
        begin(goes(t))

    for t in PAIR:
        end(goes(tiles - AHEAD + t))


def layer1_kernel(a1_ref, a1t_ref, dy_ref, wg_ref, wu_ref, wd_ref, grad_ref, act1_ref, dg_ref, du_ref,
                  wg, wu, wd, act, dgate, dup, out_g, out_u, out_d, w_sem, o_sem, d_sem, a_sem, t_sem):
    weights = tiles_of(1, (wg_ref, wu_ref), wd_ref, (wg, wu), wd, w_sem)
    outs = wide_outs(grad_ref, 0, (out_g, out_u), o_sem)

    def back(j):
        pairs = both_of((dgate, dup, act.at[0, :, pl.ds(0, NB)]), (dg_ref, du_ref, act1_ref))
        return [pltpu.make_async_copy(src, dst.at[:, columns(j)], t_sem.at[n]) for n, (src, dst) in pairs]

    begin(weights(0))

    @loop(N_J)
    def _(j):
        s = slot(j)
        end(weights(j))

        @pl.when(j >= 1)
        def _():
            end(back(j - 1))

        @pl.when(j >= AHEAD)
        def _():
            end(outs(j - AHEAD))

        @pl.when(j + 1 < N_J)
        def _():
            begin(weights(j + 1))

        for rows in strips():
            g = nn(a1_ref[rows, :], wg[s])
            u = nn(a1_ref[rows, :], wu[s])
            dgate[rows, :], dup[rows, :], silu = backwards(g, u, nt(dy_ref[rows, :], wd[s]))
            act[0, rows, pl.ds(0, NB)] = (silu * u).astype(BF16)
        wide_terms(a1t_ref, (dgate, dup), (out_g, out_u), s)
        begin(back(j))
        begin(outs(j))

    end(back(N_J - 1))
    for j in PAIR:
        end(outs(N_J - AHEAD + j))
    down_loop(grad_ref, RING, act1_ref, dy_ref, act, out_d, a_sem, d_sem)


def layer0_kernel(a0t_ref, h_ref, dy_ref, wg_ref, wu_ref, wd_ref, g_ref, u_ref, act0_ref, dg_ref, du_ref,
                  grad_ref,
                  wg, wu, wd, act, dgate, dup, out_g, out_u, out_d, gate, up, total, dh,
                  w_sem, o_sem, d_sem, a_sem, l_sem, t_sem):
    weights = tiles_of(0, (wg_ref, wu_ref), wd_ref, (wg, wu), wd, w_sem)
    outs = wide_outs(grad_ref, len(PAIR), (out_g, out_u), o_sem)
    sources = list(zip((dg_ref, du_ref), (wg_ref, wu_ref), (dgate, dup), (wg, wu), strict=True))

    def da_in(j, which):
        d_from, w_from, d_to, w_to = sources[which]
        s = slot(j)
        return [pltpu.make_async_copy(d_from.at[:, columns(j)], d_to, t_sem.at[which]),
                pltpu.make_async_copy(w_from.at[1, :, columns(j)], w_to.at[s], w_sem.at[which, s])]

    for which in PAIR:
        begin(da_in(0, which))
    total[:] = jnp.zeros_like(total)

    @loop(N_J)
    def _(j):
        for which in PAIR:
            end(da_in(j, which))
            d_to, w_to = sources[which][len(PAIR) :]
            for rows in strips():
                total[which, rows, :] += nt(d_to[rows, :], w_to[slot(j)])

            @pl.when(j + 1 < N_J)
            def _(which=which):
                begin(da_in(j + 1, which))

    begin(weights(0))

    @loop(T // STRIP)
    def _(i):
        rows = columns(i, STRIP)
        wide = h_ref[rows, :].astype(F32)
        scale = rms(wide)
        da = sum(total[which, rows, :].astype(BF16) for which in PAIR).astype(F32)
        mean = jnp.mean(da * wide, -1, keepdims=True)
        d = da * scale - wide * (mean * scale * scale * scale)
        dh[rows, :] = dy_ref[rows, :] + d.astype(BF16)

    down_loop(grad_ref, 0, act0_ref, dh, act, out_d, a_sem, d_sem)

    def products(j):
        s = slot(j)
        return [pltpu.make_async_copy(ref.at[:, columns(j)], buf.at[s], l_sem.at[n, s]) for n, (ref, buf) in both_of((g_ref, u_ref), (gate, up))]

    begin(products(0))

    @loop(N_J)
    def _(j):
        s = slot(j)
        end(weights(j))
        end(products(j))

        @pl.when(j >= AHEAD)
        def _():
            end(outs(j - AHEAD))

        @pl.when(j + 1 < N_J)
        def _():
            begin(weights(j + 1))
            begin(products(j + 1))

        for rows in strips():
            dgate[rows, :], dup[rows, :], _silu = backwards(gate[s, rows, :], up[s, rows, :], nt(dh[rows, :], wd[s]))
        wide_terms(a0t_ref, (dgate, dup), (out_g, out_u), s)
        begin(outs(j))

    for j in PAIR:
        end(outs(N_J - AHEAD + j))


def scatter_kernel(grad_ref, grad1_ref, take_ref, own_ref, ss_ref, *scratch):
    sc, rest = scatter_of((grad_ref, grad1_ref), scratch)
    enter(sc.coords, sc.core)
    sc.squares[:] = jnp.zeros_like(sc.squares)
    sc.feed(0)
    sc.feed(1)
    sc.add(0)

    @loop(UNITS + AHEAD)
    def _(i):
        sc.middles(i)

        @pl.when(i + 1 < UNITS)
        def _():
            sc.add(i + 1)

        sc.finishes(i)

        @pl.when(i + AHEAD < UNITS)
        def _():
            sc.feed(i + AHEAD)

    last_swap(sc, take_ref, own_ref, ss_ref, *rest)


TWO = len(PAIR)
OUT_TILE = (*TORUS, *CELL)
GRAD = (EACH, PARTS, CORES, *OUT_TILE)


def tile_buffers():
    return [
        *slots(BF16, (D, NB), (D, NB), (NB, D), (T, D)),
        *[pltpu.VMEM((T, NB), BF16)] * 2,
        *slots(BF16, OUT_TILE, OUT_TILE, (TWO, PARTS, CORES, TWO, RING, *CELL)),
    ]


def tile_semaphores():
    return [DMA((PARTS, TWO)), DMA((TWO, TWO)), DMA((TWO, TWO)), DMA((TWO,))]


def layer1(a1, a1t, dy, *weights):
    return pl.pallas_call(
        layer1_kernel,
        out_shape=shaped(BF16, GRAD, (T, FF), (T, FF), (T, FF)),
        in_specs=[VMEM] * 3 + [ANY] * 3,
        out_specs=(ANY,) * 4,
        scratch_shapes=[*tile_buffers(), *tile_semaphores(), DMA((PARTS,))],
        cost_estimate=pl.CostEstimate(flops=12 * T * D * FF, bytes_accessed=mib(120), transcendentals=T * FF),
        compiler_params=PARAMS(vmem_limit_bytes=mib(62)),
        name="layer1",
    )(a1, a1t, dy, *weights)


def layer0(*args):
    return pl.pallas_call(
        layer0_kernel,
        out_shape=jax.ShapeDtypeStruct(GRAD, BF16),
        in_specs=[VMEM] * 3 + [ANY] * 8,
        out_specs=ANY,
        scratch_shapes=[
            *tile_buffers(),
            *slots(F32, (T, NB), (T, NB), (T, D)),
            pltpu.VMEM((T, D), BF16),
            *tile_semaphores(),
            DMA((TWO, TWO)),
            DMA((PARTS,)),
        ],
        cost_estimate=pl.CostEstimate(flops=12 * T * D * FF, bytes_accessed=mib(200), transcendentals=T * FF),
        compiler_params=PARAMS(vmem_limit_bytes=mib(62)),
        name="layer0",
    )(*args)


def reduce_scatter(*grads):
    return pl.pallas_call(
        scatter_kernel,
        out_shape=(*shaped(BF16, (GROUP, PACKED, LANES)), *shaped(F32, (LAYERS, ROWS, D), (8, HALF))),
        in_specs=[ANY] * 2,
        out_specs=(VMEM,) * 3,
        scratch_shapes=scatter_scratch(),
        compiler_params=PARAMS(collective_id=0, has_side_effects=True, vmem_limit_bytes=mib(60)),
        name="reduce_scatter",
    )(*grads)


def adamw(w, m, v, g):
    m = 0.9 * m + 0.1 * g
    v = 0.95 * v + 0.05 * g * g
    step = m * lax.rsqrt(v + 1e-8) + 0.1 * w
    return w - 0.02 * step, m, v


def optimizer_kernel(count, take_ref, down_g_ref, squares_ref, wg_ref, wu_ref, wd_ref, mg_ref, mu_ref, md_ref, vg_ref, vu_ref, vd_ref,
                     send_ref, down_ref, mg_out, mu_out, md_out, vg_out, vu_out, vd_out, near, down_w, takes, g6, sends, sems):
    coords, core = place()
    x, y, z = coords
    copies = []
    for which, ref in enumerate((wg_ref, wu_ref)):
        copies.append(pltpu.make_async_copy(ref.at[:, pl.ds((RING * x + y) * ROWS, ROWS)], near.at[which], sems.at[which]))
    copies.append(pltpu.make_async_copy(wd_ref.at[:, pl.ds(number(coords, core) * ROWS, ROWS)], down_w, sems.at[DOWN]))
    begin(copies)
    squares = jnp.sum(jnp.sum(squares_ref[:], axis=0, keepdims=True), axis=1, keepdims=True)
    factor = jnp.minimum(1.0, 0.5 * lax.rsqrt(squares / count + 1e-30))
    takes[:] = take_ref[:].astype(F32)
    sends[:] = jnp.zeros_like(sends)
    end(copies)

    rows = lax.broadcasted_iota(jnp.int32, (GROUP, ROWS), 0)
    among = lax.broadcasted_iota(jnp.int32, (GROUP, ROWS), 1)
    sel = ((among == OWN * (CORES * z + core) + rows) & (rows < OWN)).astype(F32).astype(BF16)
    places = [(k, c, zz) for k in range(PARTS) for c in range(CORES) for zz in range(RING)]
    moments = ((mg_ref, vg_ref, mg_out, vg_out), (mu_ref, vu_ref, mu_out, vu_out))
    for layer in PAIR:
        for which in (GATE, UP):
            for half in PAIR:
                for n, (k, c, zz) in enumerate(places):
                    row = packed_row(layer, which, k)
                    g6[:, lanes(half * len(places) + n)] = takes[CORES * zz + c, pl.ds(row, OWN), lanes(half)]
            w = nn(sel, near[which, layer])[:OWN]
            m_in, v_in, m_out, v_out = moments[which]
            w, m_out[:, layer, :], v_out[:, layer, :] = adamw(w, m_in[:, layer, :], v_in[:, layer, :], g6[:] * factor)
            for n, (k, c, zz) in enumerate(places):
                sends[CORES * zz + c, pl.ds(packed_row(layer, which, k), OWN), :] = w[:, n * LANES : (n + 1) * LANES]
    send_ref[:] = sends[:].astype(BF16)
    for layer in PAIR:
        w, md_out[layer], vd_out[layer] = adamw(down_w[layer].astype(F32), md_ref[layer], vd_ref[layer], down_g_ref[layer] * factor)
        down_ref[layer] = w.astype(BF16)


def optimizer(sums, weights, m, v):
    shapes = shaped(F32, *(t.shape for t in m))
    packed = (GROUP, PACKED, LANES)
    return pl.pallas_call(
        functools.partial(optimizer_kernel, sum(w.size for w in weights)),
        out_shape=(*shaped(BF16, packed, (LAYERS, ROWS, D)), *shapes, *shapes),
        in_specs=[VMEM] * 3 + [ANY] * 3 + [VMEM] * 6,
        out_specs=(VMEM,) * 8,
        scratch_shapes=[
            *slots(BF16, (LAYERS, ROWS, FF), (ROWS, D)),
            pltpu.VMEM(packed, F32),
            pltpu.VMEM((OWN, FF), F32),
            pltpu.VMEM(packed, F32),
            DMA((PARTS,)),
        ],
        compiler_params=PARAMS(vmem_limit_bytes=mib(62)),
        name="optimizer",
    )(*sums, *weights, *m, *v)


def turned(moments):
    gate, up, down = moments
    return [gate.swapaxes(0, 1), up.swapaxes(0, 1), down]


def terms(x, dy, weights):
    g, u, act0, h, a0t, a1, a1t = forward(x, *weights)
    grad1, _act1, dg, du = layer1(a1, a1t, dy, *weights)
    return grad1, layer0(a0t, h, dy, *weights, g, u, act0, dg, du)


def local_step(x, dy, *arrays):
    weights, m, v = (arrays[i : i + PARTS] for i in range(0, len(arrays), PARTS))
    grad1, grad0 = terms(x[0], dy[0], weights)
    sums = reduce_scatter(grad0, grad1)
    send, down, *new = optimizer(sums, weights, turned(m), turned(v))
    spaces = (pltpu.VMEM, pltpu.VMEM, pltpu.VMEM, pltpu.HBM)
    gathered = all_gather(send, down)
    new_weights = put(*(pltpu.with_memory_space_constraint(w, space) for w, space in zip(gathered, spaces, strict=True)))
    return (*(n.reshape(w.shape) for n, w in zip(new_weights, weights, strict=True)), *turned(new[:PARTS]), *turned(new[PARTS:]))


def solution(mesh):
    moments = P(None, "dp", None)
    whole, mine = P(), P("dp")
    return jax.shard_map(
        local_step,
        mesh=mesh,
        in_specs=(mine, mine, whole, whole, whole, *(moments,) * 6),
        out_specs=(whole, whole, whole, *(moments,) * 6),
        check_vma=False,
    )
```

```python
import functools

import jax
import jax.numpy as jnp
from jax import lax
from jax.experimental import pallas as pl
from jax.experimental.pallas import tpu as pltpu
from jax.sharding import PartitionSpec as P

F32, BF16 = jnp.float32, jnp.bfloat16
MESH = pl.DeviceIdType.MESH
ALL = slice(None)
VMEM = pl.BlockSpec(memory_space=pltpu.VMEM)
ANY = pl.BlockSpec(memory_space=pl.ANY)
PARAMS = pltpu.CompilerParams
DMA = pltpu.SemaphoreType.DMA
SIGNALS = pltpu.SemaphoreType.REGULAR

RING, CORES, LAYERS = 4, 2, 2
TORUS = (RING, RING, RING)
AXES = range(len(TORUS))
PARTS = len(TORUS)
PAIR = range(2)
GROUP = RING * CORES
PLANE = RING * RING
OWN = 6
ROWS = OWN * GROUP
HALF = 128
LANES = 2 * HALF
T, D, FF = 1024, 768, 6144
NB = 512
N_J = FF // NB
STRIP = 256


def mib(n):
    return n << 20


def begin(copies):
    for c in copies:
        c.start()


def end(copies):
    for c in copies:
        c.wait()


def received(copies):
    for c in copies:
        c.wait_recv()


def sent(copies):
    for c in copies:
        c.wait_send()


def loop(n, first=0):
    def run(body):
        lax.fori_loop(first, n, lambda i, _: body(i), None)

    return run


def slot(i):
    return i % len(PAIR)


def columns(j, n=NB):
    return pl.ds(pl.multiple_of(j * n, n), n)


def lanes(q, n=HALF):
    return pl.ds(q * n, n)


def around(q):
    return q % RING


def place():
    p = lax.axis_index("dp")
    q = p // CORES
    return (q // PLANE, around(q // RING), around(q)), p % CORES


def number(coords, core):
    x, y, z = coords
    return ((x * RING + y) * RING + z) * CORES + core


def device(coords, core):
    return {"dp": number(coords, core)}


def moved(coords, axis, by):
    return tuple(around(q + by) if a == axis else q for a, q in enumerate(coords))


def signal(sem, where):
    pl.semaphore_signal(sem, inc=1, device_id=where, device_id_type=MESH)


def remote(src, dst, send, recv, where):
    return pltpu.make_async_remote_copy(src_ref=src, dst_ref=dst, send_sem=send, recv_sem=recv, device_id=where, device_id_type=MESH)


def group_peers(coords, core):
    x, y, z = coords
    return [((x, y, around(z + dz)), (core + dc) % CORES) for dz in range(RING) for dc in range(CORES) if dz or dc]


def plane_peers(coords, core):
    x, y, z = coords
    return [((around(x + dx), around(y + dy), z), core) for dx in range(RING) for dy in range(RING) if dx or dy]


def enter(coords, core):
    barrier = pltpu.get_barrier_semaphore()
    peers = group_peers(coords, core) + plane_peers(coords, core)
    for where, c in peers:
        signal(barrier, device(where, c))
    pl.semaphore_wait(barrier, len(peers))


GATE, UP, DOWN = range(3)
ORDER = [(1, which, half) for half in PAIR for which in (GATE, UP)]
ORDER += [(layer, DOWN, half) for layer in (1, 0) for half in PAIR]
ORDER += [(0, which, half) for half in PAIR for which in (GATE, UP)]
UNITS = len(ORDER)
UNIT = {what: u for u, what in enumerate(ORDER)}
WIDE1, DOWN1, DOWN0, WIDE0 = UNIT[1, GATE, 0], UNIT[1, DOWN, 0], UNIT[0, DOWN, 0], UNIT[0, GATE, 0]
EACH = UNITS // LAYERS
AHEAD = len(PAIR)
SIDES = ((0, 1), (1, -1))
PASSED, DIRECT = 1, 0
CELL = (ROWS, HALF)


def tile(half):
    return pl.ds(16 * half, 16 + 16 * half)


def pair_of(half):
    return pl.ds(2 * half, 2)


class Ring:
    def __init__(self, k, stage, coords, core, bufs, ss, rs, credit):
        self.axes = axes_left(k, stage)
        self.axis, self.cut = (k + stage) % PARTS, (k - 1) % PARTS
        self.last = self.axis == self.cut
        self.coords, self.core = coords, core
        self.data, self.ra, self.rb = bufs
        self.ss, self.rs, self.credit = ss, rs, credit
        self.i = coords[self.axis]

    def to(self, by):
        return device(moved(self.coords, self.axis, by), self.core)

    def index(self, place, half):
        at = [place if a == self.axis else pair_of(half) if a == self.cut else ALL for a in self.axes]
        return (*at, tile(half) if self.last else ALL, ALL)

    def landing(self, half):
        return (tile(half), ALL) if self.last else ()

    def out(self, half):
        return self.landing(half) or (*(pair_of(half) if a == self.cut else ALL for a in self.axes if a != self.axis), ALL, ALL)

    def firsts(self):
        out = {}
        for side, by in SIDES:
            for which, step, half in ((PASSED, by + by, 1 - side), (DIRECT, by, side)):
                at = self.index(around(self.i + step), half)
                n = len(out)
                out[side, which] = remote(self.data.at[at], self.ra.at[(side, which) + self.landing(half)], self.ss.at[n], self.rs.at[n], self.to(by))
        return out

    def seconds(self):
        out = []
        for side, by in SIDES:
            at, n = self.landing(1 - side), len(SIDES) * len(PAIR) + side
            out.append(remote(self.ra.at[(side, PASSED) + at], self.rb.at[(side,) + at], self.ss.at[n], self.rs.at[n], self.to(by)))
        return out

    def start(self, again):
        @pl.when(again)
        def _():
            for side, _by in SIDES:
                pl.semaphore_wait(self.credit.at[side], 1)

        begin(self.firsts().values())

    def middle(self):
        copies = self.firsts()
        for side, by in SIDES:
            half = 1 - side
            at = (side, PASSED) + self.landing(half)
            copies[side, PASSED].wait_recv()
            here = self.data[self.index(around(self.i + by), half)].astype(F32)
            self.ra[at] = (here + self.ra[at].astype(F32)).astype(BF16)
        begin(self.seconds())

    def finish(self, store, more):
        copies, passed = self.firsts(), self.seconds()
        for side, _by in SIDES:
            copies[side, DIRECT].wait_recv()
            passed[side].wait_recv()
        for half in PAIR:
            here = self.data[self.index(self.i, half)].astype(F32)
            near = self.ra[(half, DIRECT) + self.landing(half)].astype(F32)
            far = self.rb[(1 - half,) + self.landing(half)].astype(F32)
            store(self.out(half), here + near + far)
        sent([*copies.values(), *passed])

        @pl.when(more)
        def _():
            for side, by in SIDES:
                signal(self.credit.at[side], self.to(-by))


def axes_left(k, stage):
    done = [(k + s) % PARTS for s in range(stage)]
    return [a for a in AXES if a not in done]


class Scatter:
    def __init__(self, grads, bufs, sems):
        self.grads = grads
        self.coords, self.core = place()
        self.partner = device(self.coords, 1 - self.core)
        self.d1, self.r0, self.stages, self.blocks, self.squares = bufs
        self.load_sem, self.s_send, self.s_recv, self.ssem, self.rsem, self.credit, self.s_credit = sems

    def load(self, u, k, layer=0):
        src = self.grads[layer].at[u % EACH, k, self.core]
        return pltpu.make_async_copy(src, self.d1.at[slot(u), k], self.load_sem.at[slot(u), k])

    def swap(self, u, k, layer=0):
        s = slot(u)
        src = self.grads[layer].at[u % EACH, k, 1 - self.core]
        return remote(src, self.r0.at[s, k], self.s_send.at[s, k], self.s_recv.at[s, k], self.partner)

    def rings(self, u, stage):
        s = slot(u)
        return [
            Ring(k, stage, self.coords, self.core, [b.at[s] for b in self.stages[stage][k]], self.ssem.at[s, k, stage], self.rsem.at[s, k, stage],
                 self.credit.at[k, stage])
            for k in range(PARTS)
        ]

    def feed(self, u):
        @pl.when(u >= AHEAD)
        def _():
            pl.semaphore_wait(self.s_credit, 1)

        for layer, its in ((1, u < EACH), (0, u >= EACH)):

            @pl.when(its)
            def _(layer=layer):
                for k in range(PARTS):
                    begin([self.swap(u, k, layer), self.load(u, k, layer)])

    def add(self, u):
        for k in range(PARTS):
            self.load(u, k).wait()
            self.swap(u, k).wait_recv()
            d1, r0 = self.d1.at[slot(u), k], self.r0.at[slot(u), k]

            @loop(PLANE)
            def _(n, d1=d1, r0=r0):
                at = (n // RING, around(n))
                d1[at] = (d1[at].astype(F32) + r0[at].astype(F32)).astype(BF16)

        sent([self.swap(u, k) for k in range(PARTS)])

        @pl.when(u + AHEAD < UNITS)
        def _():
            signal(self.s_credit, self.partner)

        for ring in self.rings(u, 0):
            ring.start(u >= AHEAD)

    def at_stages(self, i, step):
        for stage in AXES:
            u = i - stage

            @pl.when((u >= 0) & (u < UNITS))
            def _(u=u, stage=stage):
                step(u, stage)

    def middles(self, i):
        def step(u, stage):
            for ring in self.rings(u, stage):
                ring.middle()

        self.at_stages(i, step)

    def finishes(self, i):
        def step(u, stage):
            rings = self.rings(u, stage)
            for k, ring in enumerate(rings):
                ring.finish(self.into(u, k, ring, stage), u + AHEAD < UNITS)
            if not rings[0].last:
                for ring in self.rings(u, stage + 1):
                    ring.start(u >= AHEAD)

        self.at_stages(i, step)

    def into(self, u, k, ring, stage):
        def store(at, value):
            value = value.astype(BF16)
            if not ring.last:
                self.stages[stage + 1][k][0][(slot(u),) + at] = value
                return
            self.blocks[(u, k) + at] = value
            value = value.astype(F32)
            self.squares[:] += jnp.sum((value * value).reshape(-1, *self.squares.shape), axis=0)

        return store


PACKED = 80


def packed_row(layer, which, k):
    return OWN * ((layer * len(PAIR) + which) * PARTS + k)


def scatter_scratch():
    two = (len(PAIR),)
    out = [pltpu.VMEM((*two, PARTS, *TORUS, *CELL), BF16)] * len(PAIR)
    for stage in AXES:
        for k in range(PARTS):
            left = [len(PAIR) if a == (k - 1) % PARTS else RING for a in axes_left(k, stage + 1)]
            if left:
                out.append(pltpu.VMEM((*two, *(RING for _ in left), *CELL), BF16))
            out.append(pltpu.VMEM((*two, *two, *two, *left, *CELL), BF16))
            out.append(pltpu.VMEM((*two, *two, *left, *CELL), BF16))
    each = (*two, PARTS)
    out += [pltpu.VMEM((UNITS, PARTS, *CELL), BF16), pltpu.VMEM((8, HALF), F32)]
    out += [DMA(each)] * PARTS + [DMA((*each, PARTS, 6))] * len(PAIR) + [SIGNALS((PARTS, PARTS, *two)), SIGNALS]
    out += [pltpu.VMEM((PACKED, LANES), F32), pltpu.VMEM((GROUP, PACKED, LANES), BF16), pltpu.VMEM((GROUP, PACKED, LANES), BF16)]
    out += [pltpu.VMEM((PLANE, *two, 8, HALF), F32)]
    return out + [DMA((GROUP,))] * 4 + [DMA((PLANE,))] * 2


def scatter_of(grads, scratch):
    scratch = iter(scratch)
    d1, r0 = next(scratch), next(scratch)
    stages = []
    data = [d1.at[:, k] for k in range(PARTS)]
    for stage in AXES:
        row, after = [], []
        for k in range(PARTS):
            if axes_left(k, stage + 1):
                after.append(next(scratch))
            row.append((data[k], next(scratch), next(scratch)))
        stages.append(row)
        data = after
    blocks, squares, *rest = scratch
    return Scatter(grads, (d1, r0, stages, blocks, squares), rest[:7]), rest[7:]


def last_swap(sc, out_ref, own_ref, ss_ref, stage, pack, take, sq, t_send, t_recv, q_send, q_recv, q2_send, q2_recv):
    coords, core = sc.coords, sc.core
    x, y, z = coords
    me = CORES * z + core
    first, second = (sq.at[:, i] for i in PAIR)
    peers = list(enumerate(group_peers(coords, core)))
    first[me] = sc.squares[:]
    squares = [remote(first.at[me], first.at[me], q_send.at[n], q_recv.at[n], device(where, c)) for n, (where, c) in peers]
    takes = [remote(pack.at[CORES * where[-1] + c], take.at[me], t_send.at[n], t_recv.at[n], device(where, c)) for n, (where, c) in peers]
    begin(squares)
    stage[:] = jnp.zeros_like(stage)
    for j in range(GROUP):
        for u, (layer, which, half) in enumerate(ORDER):
            for k in range(PARTS):
                if which != DOWN:
                    stage[pl.ds(packed_row(layer, which, k), OWN), lanes(half)] = sc.blocks[u, k].astype(F32)[OWN * j : OWN * j + OWN]
        pack[j] = stage[:].astype(BF16)
    begin(takes)
    for u, (layer, which, half) in enumerate(ORDER):
        for k in range(PARTS):
            if which == DOWN:
                own_ref[layer, :, lanes(half * PARTS + k)] = sc.blocks[u, k].astype(F32)
    take[me] = pack[me]
    received(squares)
    total = sum(first[j] for j in range(GROUP))
    sent(squares)
    mine = RING * x + y
    second[mine] = total
    squares = [
        remote(second.at[mine], second.at[mine], q2_send.at[n], q2_recv.at[n], device(where, c)) for n, (where, c) in enumerate(plane_peers(coords, core))
    ]
    begin(squares)
    end(takes)
    out_ref[:] = take[:]
    end(squares)
    ss_ref[:] = sum(second[j] for j in range(PLANE))


def gather_kernel(rows_ref, down_ref, wide_out, down0_out, down1_out, last_out, take, stage, t_send, t_recv, own_sem, send, recv, c_send, c_recv):
    coords, core = place()
    x, y, z = coords
    me = CORES * z + core
    partner = device(coords, 1 - core)
    enter(coords, core)
    swaps = []
    for n, (where, c) in enumerate(group_peers(coords, core)):
        swaps.append(remote(rows_ref.at[CORES * where[-1] + c], take.at[me], t_send.at[n], t_recv.at[n], device(where, c)))
    begin(swaps)
    take[me] = rows_ref[me]
    here = (*coords, core)
    own = pltpu.make_async_copy(down_ref.at[1, :, lanes(PARTS - 1, LANES)], last_out.at[here], own_sem)
    own.start()
    down0_out[here] = down_ref[0]
    down1_out[here] = down_ref[1, :, pl.ds(0, D - LANES)]

    def piece(which, k, layer, spot):
        at = tuple(ALL if q is None else q for q in spot)
        if which == DOWN:
            if layer and k == PARTS - 1:
                return last_out.at[(*at, core)]
            return (down0_out, down1_out)[layer].at[(*at, core, ALL, lanes(k, LANES))]
        base = (k * GROUP + core * RING) * LANES
        many = RING if spot[-1] is None else 1
        if many == 1:
            base += spot[-1] * LANES
        return wide_out.at[(layer, which, *at[:-1], ALL, pl.ds(pl.multiple_of(base, many * LANES), many * LANES))]

    received(swaps)
    for j in range(GROUP):
        rows = take[j].astype(F32)
        for q in range(len(stage)):
            stage[q, pl.ds(OWN * j, OWN), :] = rows[OWN * q : OWN * q + OWN]
    for layer in PAIR:
        for which in (GATE, UP):
            for k in range(PARTS):
                at = pl.multiple_of((GROUP * k + RING * core + z) * LANES, LANES)
                wide_out[layer, which, x, y, :, pl.ds(at, LANES)] = stage[packed_row(layer, which, k) // OWN].astype(BF16)
    sent(swaps)
    own.wait()

    def spot(k, turn, by):
        out = []
        for a in AXES:
            its = (k - 1 - a) % PARTS
            out.append(None if its < turn else around(coords[a] + by) if its == turn else coords[a])
        return out

    shares = []

    def share(which, k, layer, turn, by, n):
        ref = piece(which, k, layer, spot(k, turn, by))
        shares.append(remote(ref, ref, c_send.at[k, turn, which, n], c_recv.at[k, turn, which, n], partner))
        shares[-1].start()

    everything = [(which, k, side, by) for which in (GATE, UP, DOWN) for k in range(PARTS) for side, by in SIDES]
    for turn in AXES:

        def copy(which, k, by, n, layer, start):
            ref = piece(which, k, layer, spot(k, turn, start))
            sems = send.at[k, turn, which, n], recv.at[k, turn, which, n]
            return remote(ref, ref, *sems, device(moved(coords, (k - 1 - turn) % PARTS, by), core))

        first = [copy(which, k, by, side, side, 0) for which, k, side, by in everything]
        other = [copy(which, k, by, 2 + side, 1 - side, 0) for which, k, side, by in everything]
        far = [copy(which, k, by, 4 + side, side, -by) for which, k, side, by in everything]
        begin(first)
        begin(other)
        if turn == 0:
            for which, k, side, by in everything:
                share(which, k, side, turn, 0, side)
        for n, (which, k, side, by) in enumerate(everything):
            first[n].wait_recv()
            far[n].start()
            share(which, k, side, turn, -by, 2 + side)
        for n, (which, k, side, by) in enumerate(everything):
            other[n].wait_recv()
            share(which, k, 1 - side, turn, -by, 4 + side)
        for n, (which, k, side, by) in enumerate(everything):
            far[n].wait_recv()
            share(which, k, side, turn, 2, 6 + side)
        sent(first + other + far)
    end(shares)


def all_gather(rows, down):
    owners = (*TORUS, CORES, ROWS)
    return pl.pallas_call(
        gather_kernel,
        out_shape=(
            pltpu.VMEM((LAYERS, len(PAIR), RING, RING, ROWS, FF), BF16),
            pltpu.VMEM((*owners, D), BF16),
            pltpu.VMEM((*owners, D - LANES), BF16),
            jax.ShapeDtypeStruct((*owners, LANES), BF16),
        ),
        in_specs=[VMEM] * 2,
        out_specs=(VMEM, VMEM, VMEM, ANY),
        scratch_shapes=[
            pltpu.VMEM(rows.shape, BF16),
            pltpu.VMEM((LAYERS * len(PAIR) * PARTS, ROWS, LANES), F32),
            *[DMA((GROUP,))] * 2,
            DMA,
            *[DMA((PARTS, PARTS, PARTS, 6))] * 2,
            *[DMA((PARTS, PARTS, PARTS, 8))] * 2,
        ],
        compiler_params=PARAMS(collective_id=1, has_side_effects=True, vmem_limit_bytes=mib(4)),
        name="all_gather",
    )(rows, down)


def put_kernel(wide_ref, down0_ref, down1_ref, last_ref, gate_out, up_out, down_out, bounce, sems):
    def into(ref, start, n):
        return ref.at[(1, *(ALL for _ in bounce.shape[:-1]), pl.ds(start, n))]

    pairs = [(wide_ref.at[layer, which], out.at[layer]) for layer in PAIR for which, out in ((GATE, gate_out), (UP, up_out))]
    pairs += [(down0_ref, down_out.at[0]), (down1_ref, into(down_out, 0, D - LANES))]
    pairs += [(last_ref, bounce), (bounce, into(down_out, D - LANES, LANES))]
    *copies, come, go = [pltpu.make_async_copy(src, dst, sems.at[n]) for n, (src, dst) in enumerate(pairs)]
    come.start()
    begin(copies)
    come.wait()
    go.start()
    end(copies)
    go.wait()


def put(wide, down0, down1, last):
    wide_shape = jax.ShapeDtypeStruct((LAYERS, *wide.shape[2:]), BF16)
    return pl.pallas_call(
        put_kernel,
        out_shape=(wide_shape, wide_shape, jax.ShapeDtypeStruct((LAYERS, *down0.shape), BF16)),
        in_specs=[VMEM, VMEM, VMEM, ANY],
        out_specs=(ANY, ANY, ANY),
        scratch_shapes=[pltpu.VMEM(last.shape, BF16), DMA((GROUP,))],
        compiler_params=PARAMS(vmem_limit_bytes=mib(4)),
        name="put",
    )(wide, down0, down1, last)


def nn(a, b):
    return jnp.dot(a, b, preferred_element_type=F32)


def nt(a, b):
    return lax.dot_general(a, b, (((1,), (1,)), ((), ())), preferred_element_type=F32)


def tn(a, b):
    return lax.dot_general(a, b, (((0,), (0,)), ((), ())), preferred_element_type=F32)


def rms(wide):
    return lax.rsqrt(jnp.mean(wide * wide, -1, keepdims=True) + 1e-6)


def sigmoid(g):
    return 0.5 * jnp.tanh(0.5 * g) + 0.5


def strips():
    return [pl.ds(r, STRIP) for r in range(0, T, STRIP)]


def factors(g, u):
    sig = sigmoid(g)
    silu = g * sig
    return u * (sig + silu * (1 - sig)), silu, (silu * u).astype(BF16)


def forward_kernel(x_ref, wg_ref, wu_ref, wd_ref, g_ref, u_ref, act_ref, h_ref, scale_ref, a0t_ref, a1_ref, a1t_ref,
                   a0, wg, wu, wd, gate, up, act, w_sem, d_sem, g_sem, a_sem):
    def weights(j):
        s = slot(j)
        return [pltpu.make_async_copy(ref.at[0, :, columns(j)], buf.at[s], w_sem.at[n, s]) for n, (ref, buf) in enumerate(((wg_ref, wg), (wu_ref, wu)))]

    def downs(n):
        return [pltpu.make_async_copy(wd_ref.at[0, :, columns(n, LANES)], wd.at[slot(n)], d_sem.at[slot(n)])]

    def stores(j):
        s = slot(j)
        out = [pltpu.make_async_copy(buf.at[s], ref.at[:, columns(j)], g_sem.at[n, s]) for n, (ref, buf) in enumerate(((g_ref, gate), (u_ref, up)))]
        return out + [pltpu.make_async_copy(act.at[:, columns(j)], act_ref.at[:, columns(j)], a_sem.at[s])]

    def norm(from_ref, to_ref, turned_ref):
        @loop(T // STRIP)
        def _(i):
            rows = columns(i, STRIP)
            wide = from_ref[rows, :].astype(F32)
            scale = rms(wide)
            scale_ref[rows, :] = jnp.broadcast_to(scale, (STRIP, HALF))
            a = (wide * scale).astype(BF16)
            to_ref[rows, :] = a
            turned_ref[:, rows] = a.T

    begin(weights(0))
    begin(downs(0))
    norm(x_ref, a0, a0t_ref)

    @loop(N_J)
    def _(j):
        s = slot(j)
        end(weights(j))

        @pl.when(j >= AHEAD)
        def _():
            end(stores(j - AHEAD))

        @pl.when(j + 1 < N_J)
        def _():
            begin(weights(j + 1))

        for rows in strips():
            gate[s, rows, :], up[s, rows, :], act[rows, columns(j)] = factors(nn(a0[rows, :], wg[s]), nn(a0[rows, :], wu[s]))
        begin(stores(j))

    @loop(D // LANES)
    def _(n):
        end(downs(n))

        @pl.when(n + 1 < D // LANES)
        def _():
            begin(downs(n + 1))

        for r in range(0, T, NB):
            rows = pl.ds(r, NB)
            y = nn(act[rows, :], wd[slot(n)]).astype(BF16)
            h_ref[rows, columns(n, LANES)] = x_ref[rows, columns(n, LANES)] + y

    norm(h_ref, a1_ref, a1t_ref)
    for j in PAIR:
        end(stores(N_J - AHEAD + j))


def shaped(dtype, *shapes):
    return tuple(jax.ShapeDtypeStruct(s, dtype) for s in shapes)


def slots(dtype, *shapes):
    return [pltpu.VMEM((len(PAIR), *s), dtype) for s in shapes]


def forward(x, *weights):
    two = len(PAIR)
    return pl.pallas_call(
        forward_kernel,
        out_shape=(*shaped(F32, (T, FF), (T, FF)), *shaped(BF16, (T, FF), (T, D)), *shaped(F32, (T, HALF)), *shaped(BF16, (D, T), (T, D), (D, T))),
        in_specs=[VMEM, ANY, ANY, ANY],
        out_specs=(ANY,) * 3 + (VMEM,) * 5,
        scratch_shapes=[
            pltpu.VMEM((T, D), BF16),
            *slots(BF16, (D, NB), (D, NB), (FF, LANES)),
            *slots(F32, (T, NB), (T, NB)),
            pltpu.VMEM((T, FF), BF16),
            DMA((two, two)),
            DMA((two,)),
            DMA((two, two)),
            DMA((two,)),
        ],
        cost_estimate=pl.CostEstimate(flops=6 * T * D * FF, bytes_accessed=mib(100), transcendentals=T * FF),
        compiler_params=PARAMS(vmem_limit_bytes=mib(62)),
        name="forward",
    )(x, *weights)


def both_of(a, b):
    return tuple(enumerate(zip(a, b, strict=True)))


def tiles_of(layer, wide_refs, down_ref, wide_bufs, down_buf, sem):
    def copies(j):
        s = slot(j)
        wide = [pltpu.make_async_copy(ref.at[layer, :, columns(j)], buf.at[s], sem.at[n, s]) for n, (ref, buf) in both_of(wide_refs, wide_bufs)]
        return wide + [pltpu.make_async_copy(down_ref.at[layer, columns(j)], down_buf.at[s], sem.at[DOWN, s])]

    return copies


def wide_outs(grad_ref, first, bufs, sem):
    def copies(j):
        s, q = slot(j), j % EACH
        u = first + len(PAIR) * (j // EACH)
        return [pltpu.make_async_copy(buf.at[s], grad_ref.at[u + n, q // CORES, q % CORES], sem.at[n, s]) for n, buf in enumerate(bufs)]

    return copies


def wide_terms(at_ref, terms, bufs, s):
    for n, dst in enumerate(bufs):
        w = nn(at_ref[:], terms[s, n]).astype(BF16)
        for z in range(RING):
            dst[s, :, :, z] = w[:, z * HALF : (z + 1) * HALF].reshape(RING, RING, ROWS, HALF)


TILES = FF // D


def down_parts(grad_ref, first, act_hbm, d_ref, act, out, a_sem, d_sem):
    def comes(t):
        return [pltpu.make_async_copy(act_hbm.at[:, columns(t, D)], act.at[slot(t)], a_sem.at[slot(t)])]

    def goes(t):
        s = slot(t)
        x, y = t // len(PAIR), pair_of(s)
        return [pltpu.make_async_copy(out.at[s, h], grad_ref.at[first + h, :, :, x, y], d_sem.at[h, s]) for h in PAIR]

    def step(t):
        s = slot(t)
        end(comes(t))

        @pl.when(t >= AHEAD)
        def _():
            end(goes(t - AHEAD))

        @pl.when(t + 1 < TILES)
        def _():
            begin(comes(t + 1))

        w = tn(act[s], d_ref[:]).astype(BF16).reshape(len(PAIR), RING, CORES, ROWS, D)
        for h in PAIR:
            for k in range(PARTS):
                at = (h * PARTS + k) * HALF
                for c in range(CORES):
                    out[s, h, k, c] = w[:, :, c, :, at : at + HALF]
        begin(goes(t))

    def finish():
        for t in PAIR:
            end(goes(TILES - AHEAD + t))

    return comes, step, finish


def layer1_kernel(a1_ref, a1t_ref, dy_ref, wg_ref, wu_ref, wd_ref, grad_ref, act1_ref, dg_ref, du_ref,
                  wg, wu, wd, act, terms, out_g, out_u, out_d, w_sem, o_sem, d_sem, a_sem, t_sem):
    weights = tiles_of(1, (wg_ref, wu_ref), wd_ref, (wg, wu), wd, w_sem)
    outs = wide_outs(grad_ref, 0, (out_g, out_u), o_sem)

    def back(j):
        s = slot(j)
        pairs = both_of((terms.at[s, GATE], terms.at[s, UP], act.at[s, :, pl.ds(0, NB)]), (dg_ref, du_ref, act1_ref))
        return [pltpu.make_async_copy(src, dst.at[:, columns(j)], t_sem.at[n, s]) for n, (src, dst) in pairs]

    begin(weights(0))

    @loop(N_J)
    def _(j):
        s = slot(j)
        end(weights(j))

        @pl.when(j >= AHEAD)
        def _():
            end(back(j - AHEAD))
            end(outs(j - AHEAD))

        @pl.when(j + 1 < N_J)
        def _():
            begin(weights(j + 1))

        for rows in strips():
            by_gate, by_up, a = factors(nn(a1_ref[rows, :], wg[s]), nn(a1_ref[rows, :], wu[s]))
            d = nt(dy_ref[rows, :], wd[s]).astype(BF16).astype(F32)
            act[s, rows, pl.ds(0, NB)] = a
            terms[s, GATE, rows, :] = (d * by_gate).astype(BF16)
            terms[s, UP, rows, :] = (d * by_up).astype(BF16)
        wide_terms(a1t_ref, terms, (out_g, out_u), s)
        begin(back(j))
        begin(outs(j))

    for j in PAIR:
        end(back(N_J - AHEAD + j))
        end(outs(N_J - AHEAD + j))
    comes, step, finish = down_parts(grad_ref, RING, act1_ref, dy_ref, act, out_d, a_sem, d_sem)
    begin(comes(0))
    loop(TILES)(step)
    finish()


FIRST_DOWN = N_J
FIRST_WIDE = FIRST_DOWN + TILES
LAST_STEPS = FIRST_WIDE + N_J
STEPS = LAST_STEPS + 6
MIDDLES = (3, 7, 11, 17, 20, 22, 25, 28, 31, *range(LAST_STEPS + 1, STEPS))
FINISHES = (5, 9, 13, 19, 21, 23, 26, 29, *range(LAST_STEPS, STEPS))
FEEDS = (5, 9, 13, 19, 21, 23, 27, 29, LAST_STEPS, LAST_STEPS + 1)


def due(step, steps, do):
    now = functools.reduce(jnp.logical_or, [step == at for at in steps])
    n = sum((step > at).astype(jnp.int32) for at in steps)

    @pl.when(now)
    def _():
        do(n)


def layer0_kernel(a0t_ref, h_ref, scale_ref, dy_ref, wg_ref, wu_ref, wd_ref, g_ref, u_ref, act0_ref, dg_ref, du_ref, grad1_ref,
                  grad_ref, take_ref, own_ref, ss_ref,
                  wg, wu, wd, act, terms, out_g, out_u, out_d, gate, up, total, dh,
                  w_sem, o_sem, d_sem, a_sem, l_sem, t_sem, *scratch):
    sc, rest = scatter_of((grad_ref, grad1_ref), scratch)
    weights = tiles_of(0, (wg_ref, wu_ref), wd_ref, (wg, wu), wd, w_sem)
    outs = wide_outs(grad_ref, len(PAIR), (out_g, out_u), o_sem)
    comes, down_step, down_finish = down_parts(grad_ref, 0, act0_ref, dh, act, out_d, a_sem, d_sem)
    sources = both_of((dg_ref, du_ref), zip((wg_ref, wu_ref), (wg, wu), strict=True))

    def products(j):
        s = slot(j)
        return [pltpu.make_async_copy(ref.at[:, columns(j)], buf.at[s], l_sem.at[n, s]) for n, (ref, buf) in both_of((g_ref, u_ref), (gate, up))]

    def da_in(j):
        s, out = slot(j), []
        for n, (d_from, (w_from, w_to)) in sources:
            out.append(pltpu.make_async_copy(d_from.at[:, columns(j)], terms.at[s, n], t_sem.at[n, s]))
            out.append(pltpu.make_async_copy(w_from.at[1, :, columns(j)], w_to.at[s], w_sem.at[n, s]))
        return out

    def da_step(j):
        s = slot(j)
        end(da_in(j))

        @pl.when(j + 1 < N_J)
        def _():
            begin(da_in(j + 1))

        for n, (_d, (_w, w)) in sources:
            for rows in strips():
                total[n, rows, :] += nt(terms[s, n, rows, :], w[s])

    def states_step():
        @loop(T // STRIP)
        def _(i):
            rows = columns(i, STRIP)
            wide = h_ref[rows, :].astype(F32)
            scale = scale_ref[rows, pl.ds(0, 1)]
            da = sum(total[n, rows, :].astype(BF16) for n in PAIR).astype(F32)
            mean = jnp.sum(da * wide, -1, keepdims=True) * (1 / D)
            d = da * scale - wide * (mean * scale * scale * scale)
            dh[rows, :] = dy_ref[rows, :] + d.astype(BF16)

    def wide_step(j):
        s = slot(j)
        end(weights(j))
        end(products(j))

        @pl.when(j >= AHEAD)
        def _():
            end(outs(j - AHEAD))

        @pl.when(j + 1 < N_J)
        def _():
            begin(weights(j + 1))
            begin(products(j + 1))

        for rows in strips():
            d = nt(dh[rows, :], wd[s]).astype(BF16).astype(F32)
            terms[s, GATE, rows, :] = (d * gate[s, rows, :]).astype(BF16)
            terms[s, UP, rows, :] = (d * up[s, rows, :]).astype(BF16)
        wide_terms(a0t_ref, terms, (out_g, out_u), s)
        begin(outs(j))

    begin(da_in(0))
    begin(comes(0))
    begin(products(0))
    enter(sc.coords, sc.core)
    sc.squares[:] = jnp.zeros_like(sc.squares)
    sc.feed(0)
    sc.feed(1)
    total[:] = jnp.zeros_like(total)
    sc.add(0)

    @loop(STEPS)
    def _(step):
        @pl.when(step < FIRST_DOWN)
        def _():
            da_step(step)

        @pl.when(step == FIRST_DOWN - 1)
        def _():
            begin(weights(0))
            states_step()

        @pl.when((step >= FIRST_DOWN) & (step < FIRST_WIDE))
        def _():
            down_step(step - FIRST_DOWN)

        @pl.when(step == FIRST_WIDE - 1)
        def _():
            down_finish()

        @pl.when((step >= FIRST_WIDE) & (step < LAST_STEPS))
        def _():
            wide_step(step - FIRST_WIDE)

        @pl.when(step == LAST_STEPS - 1)
        def _():
            for j in PAIR:
                end(outs(N_J - AHEAD + j))

        def middles_and_add(i):
            sc.middles(i)

            @pl.when(i + 1 < UNITS)
            def _():
                sc.add(i + 1)

        due(step, MIDDLES, middles_and_add)
        due(step, FINISHES, sc.finishes)
        due(step, FEEDS, lambda n: sc.feed(n + AHEAD))

    last_swap(sc, take_ref, own_ref, ss_ref, *rest)


TWO = len(PAIR)
OUT_TILE = (*TORUS, *CELL)
GRAD = (EACH, PARTS, CORES, *OUT_TILE)


def tile_buffers():
    return [
        *slots(BF16, (D, NB), (D, NB), (NB, D), (T, D), (TWO, T, NB)),
        *slots(BF16, OUT_TILE, OUT_TILE, (TWO, PARTS, CORES, TWO, RING, *CELL)),
    ]


def tile_semaphores():
    return [DMA((PARTS, TWO)), DMA((TWO, TWO)), DMA((TWO, TWO)), DMA((TWO,))]


def layer1(a1, a1t, dy, *weights):
    return pl.pallas_call(
        layer1_kernel,
        out_shape=shaped(BF16, GRAD, (T, FF), (T, FF), (T, FF)),
        in_specs=[VMEM] * 3 + [ANY] * 3,
        out_specs=(ANY,) * 4,
        scratch_shapes=[*tile_buffers(), *tile_semaphores(), DMA((PARTS, TWO))],
        cost_estimate=pl.CostEstimate(flops=12 * T * D * FF, bytes_accessed=mib(120), transcendentals=T * FF),
        compiler_params=PARAMS(vmem_limit_bytes=mib(62)),
        name="layer1",
    )(a1, a1t, dy, *weights)


def layer0(*args):
    return pl.pallas_call(
        layer0_kernel,
        out_shape=(*shaped(BF16, GRAD, (GROUP, PACKED, LANES)), *shaped(F32, (LAYERS, ROWS, D), (8, HALF))),
        in_specs=[VMEM] * 4 + [ANY] * 9,
        out_specs=(ANY, VMEM, VMEM, VMEM),
        scratch_shapes=[
            *tile_buffers(),
            *slots(F32, (T, NB), (T, NB), (T, D)),
            pltpu.VMEM((T, D), BF16),
            *tile_semaphores(),
            DMA((TWO, TWO)),
            DMA((TWO, TWO)),
            *scatter_scratch(),
        ],
        cost_estimate=pl.CostEstimate(flops=12 * T * D * FF, bytes_accessed=mib(200), transcendentals=T * FF),
        compiler_params=PARAMS(collective_id=0, has_side_effects=True, vmem_limit_bytes=mib(63)),
        name="layer0",
    )(*args)


def adamw(w, m, v, g):
    m = 0.9 * m + 0.1 * g
    v = 0.95 * v + 0.05 * g * g
    step = m * lax.rsqrt(v + 1e-8) + 0.1 * w
    return w - 0.02 * step, m, v


def optimizer_kernel(count, take_ref, down_g_ref, squares_ref, wg_ref, wu_ref, wd_ref, mg_ref, mu_ref, md_ref, vg_ref, vu_ref, vd_ref,
                     send_ref, down_ref, mg_out, mu_out, md_out, vg_out, vu_out, vd_out, near, down_w, takes, g6, sends, sems):
    coords, core = place()
    x, y, z = coords
    copies = []
    for which, ref in enumerate((wg_ref, wu_ref)):
        copies.append(pltpu.make_async_copy(ref.at[:, pl.ds((RING * x + y) * ROWS, ROWS)], near.at[which], sems.at[which]))
    copies.append(pltpu.make_async_copy(wd_ref.at[:, pl.ds(number(coords, core) * ROWS, ROWS)], down_w, sems.at[DOWN]))
    begin(copies)
    squares = jnp.sum(jnp.sum(squares_ref[:], axis=0, keepdims=True), axis=1, keepdims=True)
    factor = jnp.minimum(1.0, 0.5 * lax.rsqrt(squares / count + 1e-30))
    takes[:] = take_ref[:].astype(F32)
    sends[:] = jnp.zeros_like(sends)
    end(copies)

    rows = lax.broadcasted_iota(jnp.int32, (GROUP, ROWS), 0)
    among = lax.broadcasted_iota(jnp.int32, (GROUP, ROWS), 1)
    sel = ((among == OWN * (CORES * z + core) + rows) & (rows < OWN)).astype(F32).astype(BF16)
    places = [(k, c, zz) for k in range(PARTS) for c in range(CORES) for zz in range(RING)]
    moments = ((mg_ref, vg_ref, mg_out, vg_out), (mu_ref, vu_ref, mu_out, vu_out))
    for layer in PAIR:
        for which in (GATE, UP):
            for half in PAIR:
                for n, (k, c, zz) in enumerate(places):
                    row = packed_row(layer, which, k)
                    g6[:, lanes(half * len(places) + n)] = takes[CORES * zz + c, pl.ds(row, OWN), lanes(half)]
            w = nn(sel, near[which, layer])[:OWN]
            m_in, v_in, m_out, v_out = moments[which]
            w, m_out[:, layer, :], v_out[:, layer, :] = adamw(w, m_in[:, layer, :], v_in[:, layer, :], g6[:] * factor)
            for n, (k, c, zz) in enumerate(places):
                sends[CORES * zz + c, pl.ds(packed_row(layer, which, k), OWN), :] = w[:, n * LANES : (n + 1) * LANES]
    send_ref[:] = sends[:].astype(BF16)
    for layer in PAIR:
        w, md_out[layer], vd_out[layer] = adamw(down_w[layer].astype(F32), md_ref[layer], vd_ref[layer], down_g_ref[layer] * factor)
        down_ref[layer] = w.astype(BF16)


def optimizer(sums, weights, m, v):
    shapes = shaped(F32, *(t.shape for t in m))
    packed = (GROUP, PACKED, LANES)
    return pl.pallas_call(
        functools.partial(optimizer_kernel, sum(w.size for w in weights)),
        out_shape=(*shaped(BF16, packed, (LAYERS, ROWS, D)), *shapes, *shapes),
        in_specs=[VMEM] * 3 + [ANY] * 3 + [VMEM] * 6,
        out_specs=(VMEM,) * 8,
        scratch_shapes=[
            *slots(BF16, (LAYERS, ROWS, FF), (ROWS, D)),
            pltpu.VMEM(packed, F32),
            pltpu.VMEM((OWN, FF), F32),
            pltpu.VMEM(packed, F32),
            DMA((PARTS,)),
        ],
        compiler_params=PARAMS(vmem_limit_bytes=mib(62)),
        name="optimizer",
    )(*sums, *weights, *m, *v)


def turned(moments):
    gate, up, down = moments
    return [gate.swapaxes(0, 1), up.swapaxes(0, 1), down]


def terms(x, dy, weights):
    by_gate, by_up, act0, h, scale, a0t, a1, a1t = forward(x, *weights)
    grad1, _act1, dg, du = layer1(a1, a1t, dy, *weights)
    return (grad1, *layer0(a0t, h, scale, dy, *weights, by_gate, by_up, act0, dg, du, grad1))


def local_step(x, dy, *arrays):
    weights, m, v = (arrays[i : i + PARTS] for i in range(0, len(arrays), PARTS))
    sums = terms(x[0], dy[0], weights)[-3:]
    send, down, *new = optimizer(sums, weights, turned(m), turned(v))
    spaces = (pltpu.VMEM, pltpu.VMEM, pltpu.VMEM, pltpu.HBM)
    gathered = all_gather(send, down)
    new_weights = put(*(pltpu.with_memory_space_constraint(w, space) for w, space in zip(gathered, spaces, strict=True)))
    return (*(n.reshape(w.shape) for n, w in zip(new_weights, weights, strict=True)), *turned(new[:PARTS]), *turned(new[PARTS:]))


def solution(mesh):
    moments = P(None, "dp", None)
    whole, mine = P(), P("dp")
    return jax.shard_map(
        local_step,
        mesh=mesh,
        in_specs=(mine, mine, whole, whole, whole, *(moments,) * 6),
        out_specs=(whole, whole, whole, *(moments,) * 6),
        check_vma=False,
    )
```

```python
import functools

import jax
import jax.numpy as jnp
from jax import lax
from jax.experimental import pallas as pl
from jax.experimental.pallas import tpu as pltpu
from jax.sharding import PartitionSpec as P

F32, BF16 = jnp.float32, jnp.bfloat16
MESH = pl.DeviceIdType.MESH
ALL = slice(None)
VMEM = pl.BlockSpec(memory_space=pltpu.VMEM)
ANY = pl.BlockSpec(memory_space=pl.ANY)
PARAMS = pltpu.CompilerParams
DMA = pltpu.SemaphoreType.DMA
SIGNALS = pltpu.SemaphoreType.REGULAR

RING, CORES, LAYERS = 4, 2, 2
TORUS = (RING, RING, RING)
AXES = range(len(TORUS))
PARTS = len(TORUS)
PAIR = range(2)
GROUP = RING * CORES
PLANE = RING * RING
OWN = 6
ROWS = OWN * GROUP
HALF = 128
LANES = 2 * HALF
T, D, FF = 1024, 768, 6144
NB = 512
N_J = FF // NB
STRIP = 256


def mib(n):
    return n << 20


def begin(copies):
    for c in copies:
        c.start()


def end(copies):
    for c in copies:
        c.wait()


def received(copies):
    for c in copies:
        c.wait_recv()


def sent(copies):
    for c in copies:
        c.wait_send()


def loop(n, first=0):
    def run(body):
        lax.fori_loop(first, n, lambda i, _: body(i), None)

    return run


def slot(i):
    return i % len(PAIR)


def columns(j, n=NB):
    return pl.ds(pl.multiple_of(j * n, n), n)


def lanes(q, n=HALF):
    return pl.ds(q * n, n)


def around(q):
    return q % RING


def place():
    p = lax.axis_index("dp")
    q = p // CORES
    return (q // PLANE, around(q // RING), around(q)), p % CORES


def number(coords, core):
    x, y, z = coords
    return ((x * RING + y) * RING + z) * CORES + core


def device(coords, core):
    return {"dp": number(coords, core)}


def moved(coords, axis, by):
    return tuple(around(q + by) if a == axis else q for a, q in enumerate(coords))


def signal(sem, where):
    pl.semaphore_signal(sem, inc=1, device_id=where, device_id_type=MESH)


def remote(src, dst, send, recv, where):
    return pltpu.make_async_remote_copy(src_ref=src, dst_ref=dst, send_sem=send, recv_sem=recv, device_id=where, device_id_type=MESH)


def group_peers(coords, core):
    x, y, z = coords
    return [((x, y, around(z + dz)), (core + dc) % CORES) for dz in range(RING) for dc in range(CORES) if dz or dc]


def plane_peers(coords, core):
    x, y, z = coords
    return [((around(x + dx), around(y + dy), z), core) for dx in range(RING) for dy in range(RING) if dx or dy]


def enter(coords, core):
    barrier = pltpu.get_barrier_semaphore()
    peers = group_peers(coords, core) + plane_peers(coords, core)
    for where, c in peers:
        signal(barrier, device(where, c))
    pl.semaphore_wait(barrier, len(peers))


GATE, UP, DOWN = range(3)
ORDER = [(1, which, half) for half in PAIR for which in (GATE, UP)]
ORDER += [(layer, DOWN, half) for layer in (1, 0) for half in PAIR]
ORDER += [(0, which, half) for half in PAIR for which in (GATE, UP)]
UNITS = len(ORDER)
UNIT = {what: u for u, what in enumerate(ORDER)}
WIDE1, DOWN1, DOWN0, WIDE0 = UNIT[1, GATE, 0], UNIT[1, DOWN, 0], UNIT[0, DOWN, 0], UNIT[0, GATE, 0]
EACH = UNITS // LAYERS
AHEAD = len(PAIR)
SIDES = ((0, 1), (1, -1))
REACH = (*SIDES, (2, 2))
PASSED, DIRECT = 1, 0
CELL = (ROWS, HALF)


def pair_of(half):
    return pl.ds(2 * half, 2)


class Ring:
    def __init__(self, k, stage, coords, core, bufs, ss, rs, credit):
        self.axes = axes_left(k, stage)
        self.axis, self.cut = (k + stage) % PARTS, (k - 1) % PARTS
        self.last = self.axis == self.cut
        self.coords, self.core = coords, core
        self.data, self.ra, *self.rb = bufs
        self.ss, self.rs, self.credit = ss, rs, credit
        self.i = coords[self.axis]

    def to(self, by):
        return device(moved(self.coords, self.axis, by), self.core)

    def index(self, by, half):
        place = around(self.i + by)
        return (*(place if a == self.axis else pair_of(half) if a == self.cut else ALL for a in self.axes), ALL, ALL)

    def out(self, half):
        return (*(pair_of(half) if a == self.cut else ALL for a in self.axes if a != self.axis), ALL, ALL)

    def copy(self, n, src, dst, by):
        return remote(src, dst, self.ss.at[n], self.rs.at[n], self.to(by))

    def firsts(self):
        if self.last:
            return {n: self.copy(n, self.data.at[self.index(by, 0)], self.ra.at[n], by) for n, by in REACH}
        out = {}
        for side, by in SIDES:
            for which, step, half in ((PASSED, by + by, 1 - side), (DIRECT, by, side)):
                out[side, which] = self.copy(len(out), self.data.at[self.index(step, half)], self.ra.at[side, which], by)
        return out

    def seconds(self):
        return [self.copy(len(SIDES) * len(PAIR) + side, self.ra.at[side, PASSED], self.rb[0].at[side], by) for side, by in SIDES]

    def peers(self):
        return REACH if self.last else SIDES

    def start(self, again):
        @pl.when(again)
        def _():
            for n, _by in self.peers():
                pl.semaphore_wait(self.credit.at[n], 1)

        begin(self.firsts().values())

    def middle(self):
        copies = self.firsts()
        for side, by in SIDES:
            copies[side, PASSED].wait_recv()
            here = self.data[self.index(by, 1 - side)].astype(F32)
            self.ra[side, PASSED] = (here + self.ra[side, PASSED].astype(F32)).astype(BF16)
        begin(self.seconds())

    def finish(self, store, more):
        copies = self.firsts()
        passed = [] if self.last else self.seconds()
        if self.last:
            received(copies.values())
            store((ALL, ALL), sum(self.ra[n].astype(F32) for n, _by in REACH) + self.data[self.index(0, 0)].astype(F32))
        else:
            received([copies[side, DIRECT] for side, _by in SIDES])
            received(passed)
            for half in PAIR:
                here = self.data[self.index(0, half)].astype(F32)
                store(self.out(half), here + self.ra[half, DIRECT].astype(F32) + self.rb[0][1 - half].astype(F32))
        sent([*copies.values(), *passed])

        @pl.when(more)
        def _():
            for n, by in self.peers():
                signal(self.credit.at[n], self.to(-by))


def axes_left(k, stage):
    done = [(k + s) % PARTS for s in range(stage)]
    return [a for a in AXES if a not in done]


class Scatter:
    def __init__(self, grads, bufs, sems):
        self.grads = grads
        self.coords, self.core = place()
        self.partner = device(self.coords, 1 - self.core)
        self.d1, self.r0, self.stages, self.blocks, self.squares = bufs
        self.load_sem, self.s_send, self.s_recv, self.ssem, self.rsem, self.credit, self.s_credit = sems

    def load(self, u, k, layer=0):
        src = self.grads[layer].at[u % EACH, k, self.core]
        return pltpu.make_async_copy(src, self.d1.at[slot(u), k], self.load_sem.at[slot(u), k])

    def swap(self, u, k, layer=0):
        s = slot(u)
        src = self.grads[layer].at[u % EACH, k, 1 - self.core]
        return remote(src, self.r0.at[s, k], self.s_send.at[s, k], self.s_recv.at[s, k], self.partner)

    def rings(self, u, stage):
        s = slot(u)
        return [
            Ring(k, stage, self.coords, self.core, [b.at[s] for b in self.stages[stage][k]], self.ssem.at[s, k, stage], self.rsem.at[s, k, stage],
                 self.credit.at[k, stage])
            for k in range(PARTS)
        ]

    def start(self, u, copy):
        for layer, its in ((1, u < EACH), (0, u >= EACH)):

            @pl.when(its)
            def _(layer=layer):
                begin([copy(u, k, layer) for k in range(PARTS)])

    def start_swap(self, u):
        @pl.when(u >= AHEAD)
        def _():
            pl.semaphore_wait(self.s_credit, 1)

        self.start(u, self.swap)

    def start_load(self, u):
        self.start(u, self.load)

    def add(self, u):
        for k in range(PARTS):
            self.load(u, k).wait()
            self.swap(u, k).wait_recv()
            d1, r0 = self.d1.at[slot(u), k], self.r0.at[slot(u), k]

            @loop(PLANE)
            def _(n, d1=d1, r0=r0):
                at = (n // RING, around(n))
                d1[at] = (d1[at].astype(F32) + r0[at].astype(F32)).astype(BF16)

        sent([self.swap(u, k) for k in range(PARTS)])

        @pl.when(u + AHEAD < UNITS)
        def _():
            signal(self.s_credit, self.partner)

        for ring in self.rings(u, 0):
            ring.start(u >= AHEAD)

    def at_stages(self, i, stages, step):
        for stage in reversed(stages):
            u = i - stage

            @pl.when((u >= 0) & (u < UNITS))
            def _(u=u, stage=stage):
                step(u, stage)

    def middles(self, i):
        def step(u, stage):
            for ring in self.rings(u, stage):
                ring.middle()

        self.at_stages(i, AXES[:-1], step)

    def finishes(self, i):
        def step(u, stage):
            rings = self.rings(u, stage)
            for k, ring in enumerate(rings):
                ring.finish(self.into(u, k, ring, stage), u + AHEAD < UNITS)
            if not rings[0].last:
                for ring in self.rings(u, stage + 1):
                    ring.start(u >= AHEAD)

        self.at_stages(i, AXES, step)

    def into(self, u, k, ring, stage):
        def store(at, value):
            value = value.astype(BF16)
            if not ring.last:
                self.stages[stage + 1][k][0][(slot(u),) + at] = value
                return
            self.blocks[(u, k) + at] = value
            value = value.astype(F32)
            self.squares[:] += jnp.sum((value * value).reshape(-1, *self.squares.shape), axis=0)

        return store


PACKED = 80


def packed_row(layer, which, k):
    return OWN * ((layer * len(PAIR) + which) * PARTS + k)


def scatter_scratch():
    two = (len(PAIR),)
    out = [pltpu.VMEM((*two, PARTS, *TORUS, *CELL), BF16)] * len(PAIR)
    for stage in AXES:
        for k in range(PARTS):
            left = [len(PAIR) if a == (k - 1) % PARTS else RING for a in axes_left(k, stage + 1)]
            if left:
                out.append(pltpu.VMEM((*two, *(RING for _ in left), *CELL), BF16))
                out.append(pltpu.VMEM((*two, *two, *two, *left, *CELL), BF16))
                out.append(pltpu.VMEM((*two, *two, *left, *CELL), BF16))
            else:
                out.append(pltpu.VMEM((*two, len(REACH), *CELL), BF16))
    each = (*two, PARTS)
    out += [pltpu.VMEM((UNITS, PARTS, *CELL), BF16), pltpu.VMEM((8, HALF), F32)]
    out += [DMA(each)] * PARTS + [DMA((*each, PARTS, 6))] * len(PAIR) + [SIGNALS((PARTS, PARTS, len(REACH))), SIGNALS]
    out += [pltpu.VMEM((PACKED, LANES), F32), pltpu.VMEM((GROUP, PACKED, LANES), BF16), pltpu.VMEM((GROUP, PACKED, LANES), BF16)]
    out += [pltpu.VMEM((PLANE, *two, 8, HALF), F32)]
    return out + [DMA((GROUP,))] * 4 + [DMA((PLANE,))] * 2


def scatter_of(grads, scratch):
    scratch = iter(scratch)
    d1, r0 = next(scratch), next(scratch)
    stages = []
    data = [d1.at[:, k] for k in range(PARTS)]
    for stage in AXES:
        row, after = [], []
        for k in range(PARTS):
            own = [data[k]]
            if axes_left(k, stage + 1):
                after.append(next(scratch))
                own.append(next(scratch))
            row.append((*own, next(scratch)))
        stages.append(row)
        data = after
    blocks, squares, *rest = scratch
    return Scatter(grads, (d1, r0, stages, blocks, squares), rest[:7]), rest[7:]


def last_swap(sc, out_ref, own_ref, ss_ref, stage, pack, take, sq, t_send, t_recv, q_send, q_recv, q2_send, q2_recv):
    coords, core = sc.coords, sc.core
    x, y, z = coords
    me = CORES * z + core
    first, second = (sq.at[:, i] for i in PAIR)
    peers = list(enumerate(group_peers(coords, core)))
    first[me] = sc.squares[:]
    squares = [remote(first.at[me], first.at[me], q_send.at[n], q_recv.at[n], device(where, c)) for n, (where, c) in peers]
    takes = [remote(pack.at[CORES * where[-1] + c], take.at[me], t_send.at[n], t_recv.at[n], device(where, c)) for n, (where, c) in peers]
    begin(squares)
    stage[:] = jnp.zeros_like(stage)
    for j in range(GROUP):
        for u, (layer, which, half) in enumerate(ORDER):
            for k in range(PARTS):
                if which != DOWN:
                    stage[pl.ds(packed_row(layer, which, k), OWN), lanes(half)] = sc.blocks[u, k].astype(F32)[OWN * j : OWN * j + OWN]
        pack[j] = stage[:].astype(BF16)
    begin(takes)
    for u, (layer, which, half) in enumerate(ORDER):
        for k in range(PARTS):
            if which == DOWN:
                own_ref[layer, :, lanes(half * PARTS + k)] = sc.blocks[u, k].astype(F32)
    take[me] = pack[me]
    received(squares)
    total = sum(first[j] for j in range(GROUP))
    sent(squares)
    mine = RING * x + y
    second[mine] = total
    squares = [
        remote(second.at[mine], second.at[mine], q2_send.at[n], q2_recv.at[n], device(where, c)) for n, (where, c) in enumerate(plane_peers(coords, core))
    ]
    begin(squares)
    end(takes)
    out_ref[:] = take[:]
    end(squares)
    ss_ref[:] = sum(second[j] for j in range(PLANE))


def gather_kernel(rows_ref, down_ref, wide_out, down0_out, down1_out, last_out, take, stage, t_send, t_recv, own_sem, send, recv, c_send, c_recv):
    coords, core = place()
    x, y, z = coords
    me = CORES * z + core
    partner = device(coords, 1 - core)
    enter(coords, core)
    swaps = []
    for n, (where, c) in enumerate(group_peers(coords, core)):
        swaps.append(remote(rows_ref.at[CORES * where[-1] + c], take.at[me], t_send.at[n], t_recv.at[n], device(where, c)))
    begin(swaps)
    here = (*coords, core)
    own = pltpu.make_async_copy(down_ref.at[1, :, lanes(PARTS - 1, LANES)], last_out.at[here], own_sem)
    own.start()
    down0_out[here] = down_ref[0]
    down1_out[here] = down_ref[1, :, pl.ds(0, D - LANES)]

    def piece(which, k, layer, spot):
        at = tuple(ALL if q is None else q for q in spot)
        if which == DOWN:
            if layer and k == PARTS - 1:
                return last_out.at[(*at, core)]
            return (down0_out, down1_out)[layer].at[(*at, core, ALL, lanes(k, LANES))]
        base = (k * GROUP + core * RING) * LANES
        many = RING if spot[-1] is None else 1
        if many == 1:
            base += spot[-1] * LANES
        return wide_out.at[(layer, which, *at[:-1], ALL, pl.ds(pl.multiple_of(base, many * LANES), many * LANES))]

    def unpack():
        take[me] = rows_ref[me]
        received(swaps)
        for j in range(GROUP):
            rows = take[j].astype(F32)
            for q in range(len(stage)):
                stage[q, pl.ds(OWN * j, OWN), :] = rows[OWN * q : OWN * q + OWN]
        for layer in PAIR:
            for which in (GATE, UP):
                for k in range(PARTS):
                    at = pl.multiple_of((GROUP * k + RING * core + z) * LANES, LANES)
                    wide_out[layer, which, x, y, :, pl.ds(at, LANES)] = stage[packed_row(layer, which, k) // OWN].astype(BF16)
        sent(swaps)

    def spot(k, turn, by):
        out = []
        for a in AXES:
            its = (k - 1 - a) % PARTS
            out.append(None if its < turn else around(coords[a] + by) if its == turn else coords[a])
        return out

    shares = []

    def share(which, k, layer, turn, by, n):
        ref = piece(which, k, layer, spot(k, turn, by))
        shares.append(remote(ref, ref, c_send.at[k, turn, which, n], c_recv.at[k, turn, which, n], partner))
        shares[-1].start()

    class Turn:
        def __init__(self, matrices, turn):
            self.turn = turn
            self.all = [(which, k, side, by) for which in matrices for k in range(PARTS) for side, by in SIDES]
            self.first = [self.copy(which, k, by, side, side, 0) for which, k, side, by in self.all]
            self.other = [self.copy(which, k, by, 2 + side, 1 - side, 0) for which, k, side, by in self.all]
            self.far = [self.copy(which, k, by, 4 + side, side, -by) for which, k, side, by in self.all]

        def copy(self, which, k, by, n, layer, start):
            ref = piece(which, k, layer, spot(k, self.turn, start))
            sems = send.at[k, self.turn, which, n], recv.at[k, self.turn, which, n]
            return remote(ref, ref, *sems, device(moved(coords, (k - 1 - self.turn) % PARTS, by), core))

        def start(self):
            begin(self.first)
            begin(self.other)
            if self.turn == 0:
                for which, k, side, by in self.all:
                    share(which, k, side, self.turn, 0, side)

        def near(self):
            for n, (which, k, side, by) in enumerate(self.all):
                self.first[n].wait_recv()
                self.far[n].start()
                share(which, k, side, self.turn, -by, 2 + side)
            for n, (which, k, side, by) in enumerate(self.all):
                self.other[n].wait_recv()
                share(which, k, 1 - side, self.turn, -by, 4 + side)

        def done(self):
            for n, (which, k, side, by) in enumerate(self.all):
                self.far[n].wait_recv()
                share(which, k, side, self.turn, 2, 6 + side)
            sent(self.first + self.other + self.far)

    streams = [[Turn(matrices, turn) for matrices in ((DOWN,), (GATE, UP))] for turn in AXES]
    own.wait()
    for downs, wides in streams:
        if downs.turn == 0:
            downs.start()
            unpack()
            wides.start()
        downs.near()
        wides.near()
        for stream, now in enumerate((downs, wides)):
            now.done()
            if now.turn + 1 < len(streams):
                streams[now.turn + 1][stream].start()
    end(shares)


def all_gather(rows, down):
    owners = (*TORUS, CORES, ROWS)
    return pl.pallas_call(
        gather_kernel,
        out_shape=(
            pltpu.VMEM((LAYERS, len(PAIR), RING, RING, ROWS, FF), BF16),
            pltpu.VMEM((*owners, D), BF16),
            pltpu.VMEM((*owners, D - LANES), BF16),
            jax.ShapeDtypeStruct((*owners, LANES), BF16),
        ),
        in_specs=[VMEM] * 2,
        out_specs=(VMEM, VMEM, VMEM, ANY),
        scratch_shapes=[
            pltpu.VMEM(rows.shape, BF16),
            pltpu.VMEM((LAYERS * len(PAIR) * PARTS, ROWS, LANES), F32),
            *[DMA((GROUP,))] * 2,
            DMA,
            *[DMA((PARTS, PARTS, PARTS, 6))] * 2,
            *[DMA((PARTS, PARTS, PARTS, 8))] * 2,
        ],
        compiler_params=PARAMS(collective_id=1, has_side_effects=True, vmem_limit_bytes=mib(4)),
        name="all_gather",
    )(rows, down)


def put_kernel(wide_ref, down0_ref, down1_ref, last_ref, gate_out, up_out, down_out, bounce, sems):
    def into(ref, start, n):
        return ref.at[(1, *(ALL for _ in bounce.shape[:-1]), pl.ds(start, n))]

    pairs = [(wide_ref.at[layer, which], out.at[layer]) for layer in PAIR for which, out in ((GATE, gate_out), (UP, up_out))]
    pairs += [(down0_ref, down_out.at[0]), (down1_ref, into(down_out, 0, D - LANES))]
    pairs += [(last_ref, bounce), (bounce, into(down_out, D - LANES, LANES))]
    *copies, come, go = [pltpu.make_async_copy(src, dst, sems.at[n]) for n, (src, dst) in enumerate(pairs)]
    come.start()
    begin(copies)
    come.wait()
    go.start()
    end(copies)
    go.wait()


def put(wide, down0, down1, last):
    wide_shape = jax.ShapeDtypeStruct((LAYERS, *wide.shape[2:]), BF16)
    return pl.pallas_call(
        put_kernel,
        out_shape=(wide_shape, wide_shape, jax.ShapeDtypeStruct((LAYERS, *down0.shape), BF16)),
        in_specs=[VMEM, VMEM, VMEM, ANY],
        out_specs=(ANY, ANY, ANY),
        scratch_shapes=[pltpu.VMEM(last.shape, BF16), DMA((GROUP,))],
        compiler_params=PARAMS(vmem_limit_bytes=mib(4)),
        name="put",
    )(wide, down0, down1, last)


def nn(a, b):
    return jnp.dot(a, b, preferred_element_type=F32)


def nt(a, b):
    return lax.dot_general(a, b, (((1,), (1,)), ((), ())), preferred_element_type=F32)


def tn(a, b):
    return lax.dot_general(a, b, (((0,), (0,)), ((), ())), preferred_element_type=F32)


def rms(wide):
    return lax.rsqrt(jnp.mean(wide * wide, -1, keepdims=True) + 1e-6)


def sigmoid(g):
    return 0.5 * jnp.tanh(0.5 * g) + 0.5


def strips():
    return [pl.ds(r, STRIP) for r in range(0, T, STRIP)]


def factors(g, u):
    sig = sigmoid(g)
    silu = g * sig
    return u * (sig + silu * (1 - sig)), silu, (silu * u).astype(BF16)


def forward_kernel(x_ref, wg_ref, wu_ref, wd_ref, g_ref, u_ref, act_ref, h_ref, scale_ref, a0t_ref, a1_ref, a1t_ref,
                   a0, wg, wu, wd, gate, up, act, w_sem, d_sem, g_sem, a_sem):
    def weights(j):
        s = slot(j)
        return [pltpu.make_async_copy(ref.at[0, :, columns(j)], buf.at[s], w_sem.at[n, s]) for n, (ref, buf) in enumerate(((wg_ref, wg), (wu_ref, wu)))]

    def downs(n):
        return [pltpu.make_async_copy(wd_ref.at[0, :, columns(n, LANES)], wd.at[slot(n)], d_sem.at[slot(n)])]

    def stores(j):
        s = slot(j)
        out = [pltpu.make_async_copy(buf.at[s], ref.at[:, columns(j)], g_sem.at[n, s]) for n, (ref, buf) in enumerate(((g_ref, gate), (u_ref, up)))]
        return out + [pltpu.make_async_copy(act.at[:, columns(j)], act_ref.at[:, columns(j)], a_sem.at[s])]

    def norm(from_ref, to_ref, turned_ref):
        @loop(T // STRIP)
        def _(i):
            rows = columns(i, STRIP)
            wide = from_ref[rows, :].astype(F32)
            scale = rms(wide)
            scale_ref[rows, :] = jnp.broadcast_to(scale, (STRIP, HALF))
            a = (wide * scale).astype(BF16)
            to_ref[rows, :] = a
            turned_ref[:, rows] = a.T

    begin(weights(0))
    begin(downs(0))
    norm(x_ref, a0, a0t_ref)

    @loop(N_J)
    def _(j):
        s = slot(j)
        end(weights(j))

        @pl.when(j >= AHEAD)
        def _():
            end(stores(j - AHEAD))

        @pl.when(j + 1 < N_J)
        def _():
            begin(weights(j + 1))

        for rows in strips():
            gate[s, rows, :], up[s, rows, :], act[rows, columns(j)] = factors(nn(a0[rows, :], wg[s]), nn(a0[rows, :], wu[s]))
        begin(stores(j))

    @loop(D // LANES)
    def _(n):
        end(downs(n))

        @pl.when(n + 1 < D // LANES)
        def _():
            begin(downs(n + 1))

        for r in range(0, T, NB):
            rows = pl.ds(r, NB)
            y = nn(act[rows, :], wd[slot(n)]).astype(BF16)
            h_ref[rows, columns(n, LANES)] = x_ref[rows, columns(n, LANES)] + y

    norm(h_ref, a1_ref, a1t_ref)
    for j in PAIR:
        end(stores(N_J - AHEAD + j))


def shaped(dtype, *shapes):
    return tuple(jax.ShapeDtypeStruct(s, dtype) for s in shapes)


def slots(dtype, *shapes):
    return [pltpu.VMEM((len(PAIR), *s), dtype) for s in shapes]


def forward(x, *weights):
    two = len(PAIR)
    return pl.pallas_call(
        forward_kernel,
        out_shape=(*shaped(F32, (T, FF), (T, FF)), *shaped(BF16, (T, FF), (T, D)), *shaped(F32, (T, HALF)), *shaped(BF16, (D, T), (T, D), (D, T))),
        in_specs=[VMEM, ANY, ANY, ANY],
        out_specs=(ANY,) * 3 + (VMEM,) * 5,
        scratch_shapes=[
            pltpu.VMEM((T, D), BF16),
            *slots(BF16, (D, NB), (D, NB), (FF, LANES)),
            *slots(F32, (T, NB), (T, NB)),
            pltpu.VMEM((T, FF), BF16),
            DMA((two, two)),
            DMA((two,)),
            DMA((two, two)),
            DMA((two,)),
        ],
        cost_estimate=pl.CostEstimate(flops=6 * T * D * FF, bytes_accessed=mib(100), transcendentals=T * FF),
        compiler_params=PARAMS(vmem_limit_bytes=mib(62)),
        name="forward",
    )(x, *weights)


def both_of(a, b):
    return tuple(enumerate(zip(a, b, strict=True)))


def tiles_of(layer, wide_refs, down_ref, wide_bufs, down_buf, sem):
    def copies(j):
        s = slot(j)
        wide = [pltpu.make_async_copy(ref.at[layer, :, columns(j)], buf.at[s], sem.at[n, s]) for n, (ref, buf) in both_of(wide_refs, wide_bufs)]
        return wide + [pltpu.make_async_copy(down_ref.at[layer, columns(j)], down_buf.at[s], sem.at[DOWN, s])]

    return copies


def wide_outs(grad_ref, first, bufs, sem):
    def copies(j):
        s, q = slot(j), j % EACH
        u = first + len(PAIR) * (j // EACH)
        return [pltpu.make_async_copy(buf.at[s], grad_ref.at[u + n, q // CORES, q % CORES], sem.at[n, s]) for n, buf in enumerate(bufs)]

    return copies


def wide_terms(at_ref, terms, bufs, s):
    for n, dst in enumerate(bufs):
        w = nn(at_ref[:], terms[s, n]).astype(BF16)
        for z in range(RING):
            dst[s, :, :, z] = w[:, z * HALF : (z + 1) * HALF].reshape(RING, RING, ROWS, HALF)


TILES = FF // D


def down_parts(grad_ref, first, act_hbm, d_ref, act, out, a_sem, d_sem):
    def comes(t):
        return [pltpu.make_async_copy(act_hbm.at[:, columns(t, D)], act.at[slot(t)], a_sem.at[slot(t)])]

    def goes(t):
        s = slot(t)
        x, y = t // len(PAIR), pair_of(s)
        return [pltpu.make_async_copy(out.at[s, h], grad_ref.at[first + h, :, :, x, y], d_sem.at[h, s]) for h in PAIR]

    def step(t):
        s = slot(t)
        end(comes(t))

        @pl.when(t >= AHEAD)
        def _():
            end(goes(t - AHEAD))

        @pl.when(t + 1 < TILES)
        def _():
            begin(comes(t + 1))

        w = tn(act[s], d_ref[:]).astype(BF16).reshape(len(PAIR), RING, CORES, ROWS, D)
        for h in PAIR:
            for k in range(PARTS):
                at = (h * PARTS + k) * HALF
                for c in range(CORES):
                    out[s, h, k, c] = w[:, :, c, :, at : at + HALF]
        begin(goes(t))

    def finish():
        for t in PAIR:
            end(goes(TILES - AHEAD + t))

    return comes, step, finish


def layer1_kernel(a1_ref, a1t_ref, dy_ref, wg_ref, wu_ref, wd_ref, grad_ref, act1_ref, dg_ref, du_ref,
                  wg, wu, wd, act, terms, out_g, out_u, out_d, w_sem, o_sem, d_sem, a_sem, t_sem):
    weights = tiles_of(1, (wg_ref, wu_ref), wd_ref, (wg, wu), wd, w_sem)
    outs = wide_outs(grad_ref, 0, (out_g, out_u), o_sem)

    def back(j):
        s = slot(j)
        pairs = both_of((terms.at[s, GATE], terms.at[s, UP], act.at[s, :, pl.ds(0, NB)]), (dg_ref, du_ref, act1_ref))
        return [pltpu.make_async_copy(src, dst.at[:, columns(j)], t_sem.at[n, s]) for n, (src, dst) in pairs]

    begin(weights(0))

    @loop(N_J)
    def _(j):
        s = slot(j)
        end(weights(j))

        @pl.when(j >= AHEAD)
        def _():
            end(back(j - AHEAD))
            end(outs(j - AHEAD))

        @pl.when(j + 1 < N_J)
        def _():
            begin(weights(j + 1))

        for rows in strips():
            by_gate, by_up, a = factors(nn(a1_ref[rows, :], wg[s]), nn(a1_ref[rows, :], wu[s]))
            d = nt(dy_ref[rows, :], wd[s]).astype(BF16).astype(F32)
            act[s, rows, pl.ds(0, NB)] = a
            terms[s, GATE, rows, :] = (d * by_gate).astype(BF16)
            terms[s, UP, rows, :] = (d * by_up).astype(BF16)
        wide_terms(a1t_ref, terms, (out_g, out_u), s)
        begin(back(j))
        begin(outs(j))

    for j in PAIR:
        end(back(N_J - AHEAD + j))
        end(outs(N_J - AHEAD + j))
    comes, step, finish = down_parts(grad_ref, RING, act1_ref, dy_ref, act, out_d, a_sem, d_sem)
    begin(comes(0))
    loop(TILES)(step)
    finish()


FIRST_DOWN = N_J
FIRST_WIDE = FIRST_DOWN + TILES
LAST_STEPS = FIRST_WIDE + N_J
STEPS = LAST_STEPS + 6
MIDDLES = (4, 8, 11, 15, 21, 23, 25, 27, 30, *range(LAST_STEPS + 1, STEPS - 1))
ADDS = (2, 3, 8, 11, 14, 21, 23, 25, 28, 29, LAST_STEPS + 1, LAST_STEPS + 2)
FINISHES = (7, 10, 13, 20, 22, 24, 26, 28, *range(LAST_STEPS, STEPS))
LOADS = FINISHES[: UNITS - AHEAD]
SWAPS = (2, 3, 8, 11, 19, 21, 26, 27, LAST_STEPS - 1, LAST_STEPS)


def due(step, steps, do):
    now = functools.reduce(jnp.logical_or, [step == at for at in steps])
    n = sum((step > at).astype(jnp.int32) for at in steps)

    @pl.when(now)
    def _():
        do(n)


def layer0_kernel(a0t_ref, h_ref, scale_ref, dy_ref, wg_ref, wu_ref, wd_ref, g_ref, u_ref, act0_ref, dg_ref, du_ref, grad1_ref,
                  grad_ref, take_ref, own_ref, ss_ref,
                  wg, wu, wd, act, terms, out_g, out_u, out_d, gate, up, total, dh,
                  w_sem, o_sem, d_sem, a_sem, l_sem, t_sem, *scratch):
    sc, rest = scatter_of((grad_ref, grad1_ref), scratch)
    weights = tiles_of(0, (wg_ref, wu_ref), wd_ref, (wg, wu), wd, w_sem)
    outs = wide_outs(grad_ref, len(PAIR), (out_g, out_u), o_sem)
    comes, down_step, down_finish = down_parts(grad_ref, 0, act0_ref, dh, act, out_d, a_sem, d_sem)
    sources = both_of((dg_ref, du_ref), zip((wg_ref, wu_ref), (wg, wu), strict=True))

    def products(j):
        s = slot(j)
        return [pltpu.make_async_copy(ref.at[:, columns(j)], buf.at[s], l_sem.at[n, s]) for n, (ref, buf) in both_of((g_ref, u_ref), (gate, up))]

    def da_in(j):
        s, out = slot(j), []
        for n, (d_from, (w_from, w_to)) in sources:
            out.append(pltpu.make_async_copy(d_from.at[:, columns(j)], terms.at[s, n], t_sem.at[n, s]))
            out.append(pltpu.make_async_copy(w_from.at[1, :, columns(j)], w_to.at[s], w_sem.at[n, s]))
        return out

    def da_step(j):
        s = slot(j)
        end(da_in(j))

        @pl.when(j + 1 < N_J)
        def _():
            begin(da_in(j + 1))

        for n, (_d, (_w, w)) in sources:
            for rows in strips():
                total[n, rows, :] += nt(terms[s, n, rows, :], w[s])

    def states_step():
        @loop(T // STRIP)
        def _(i):
            rows = columns(i, STRIP)
            wide = h_ref[rows, :].astype(F32)
            scale = scale_ref[rows, pl.ds(0, 1)]
            da = sum(total[n, rows, :].astype(BF16) for n in PAIR).astype(F32)
            mean = jnp.sum(da * wide, -1, keepdims=True) * (1 / D)
            d = da * scale - wide * (mean * scale * scale * scale)
            dh[rows, :] = dy_ref[rows, :] + d.astype(BF16)

    def wide_step(j):
        s = slot(j)
        end(weights(j))
        end(products(j))

        @pl.when(j + 1 < N_J)
        def _():
            begin(weights(j + 1))
            begin(products(j + 1))

        for rows in strips():
            d = nt(dh[rows, :], wd[s]).astype(BF16).astype(F32)
            terms[s, GATE, rows, :] = (d * gate[s, rows, :]).astype(BF16)
            terms[s, UP, rows, :] = (d * up[s, rows, :]).astype(BF16)
        wide_terms(a0t_ref, terms, (out_g, out_u), s)

        @pl.when(j >= 1)
        def _():
            end(outs(j - 1))

        begin(outs(j))

    begin(da_in(0))
    begin(comes(0))
    begin(products(0))
    enter(sc.coords, sc.core)
    sc.squares[:] = jnp.zeros_like(sc.squares)
    for u in range(AHEAD):
        sc.start_swap(u)
        sc.start_load(u)
    total[:] = jnp.zeros_like(total)

    @loop(STEPS)
    def _(step):
        @pl.when(step < FIRST_DOWN)
        def _():
            da_step(step)

        @pl.when(step == FIRST_DOWN - 1)
        def _():
            begin(weights(0))
            states_step()

        @pl.when((step >= FIRST_DOWN) & (step < FIRST_WIDE))
        def _():
            down_step(step - FIRST_DOWN)

        @pl.when(step == FIRST_WIDE - 1)
        def _():
            down_finish()

        @pl.when((step >= FIRST_WIDE) & (step < LAST_STEPS))
        def _():
            wide_step(step - FIRST_WIDE)

        @pl.when(step == LAST_STEPS - 1)
        def _():
            end(outs(N_J - 1))

        due(step, MIDDLES, sc.middles)
        due(step, ADDS, sc.add)
        due(step, FINISHES, sc.finishes)
        due(step, LOADS, lambda n: sc.start_load(n + AHEAD))
        due(step, SWAPS, lambda n: sc.start_swap(n + AHEAD))

    last_swap(sc, take_ref, own_ref, ss_ref, *rest)


TWO = len(PAIR)
OUT_TILE = (*TORUS, *CELL)
GRAD = (EACH, PARTS, CORES, *OUT_TILE)


def tile_buffers():
    return [
        *slots(BF16, (D, NB), (D, NB), (NB, D), (T, D), (TWO, T, NB)),
        *slots(BF16, OUT_TILE, OUT_TILE, (TWO, PARTS, CORES, TWO, RING, *CELL)),
    ]


def tile_semaphores():
    return [DMA((PARTS, TWO)), DMA((TWO, TWO)), DMA((TWO, TWO)), DMA((TWO,))]


def layer1(a1, a1t, dy, *weights):
    return pl.pallas_call(
        layer1_kernel,
        out_shape=shaped(BF16, GRAD, (T, FF), (T, FF), (T, FF)),
        in_specs=[VMEM] * 3 + [ANY] * 3,
        out_specs=(ANY,) * 4,
        scratch_shapes=[*tile_buffers(), *tile_semaphores(), DMA((PARTS, TWO))],
        cost_estimate=pl.CostEstimate(flops=12 * T * D * FF, bytes_accessed=mib(120), transcendentals=T * FF),
        compiler_params=PARAMS(vmem_limit_bytes=mib(62)),
        name="layer1",
    )(a1, a1t, dy, *weights)


def layer0(*args):
    return pl.pallas_call(
        layer0_kernel,
        out_shape=(*shaped(BF16, GRAD, (GROUP, PACKED, LANES)), *shaped(F32, (LAYERS, ROWS, D), (8, HALF))),
        in_specs=[VMEM] * 4 + [ANY] * 9,
        out_specs=(ANY, VMEM, VMEM, VMEM),
        scratch_shapes=[
            *tile_buffers(),
            *slots(F32, (T, NB), (T, NB), (T, D)),
            pltpu.VMEM((T, D), BF16),
            *tile_semaphores(),
            DMA((TWO, TWO)),
            DMA((TWO, TWO)),
            *scatter_scratch(),
        ],
        cost_estimate=pl.CostEstimate(flops=12 * T * D * FF, bytes_accessed=mib(200), transcendentals=T * FF),
        compiler_params=PARAMS(collective_id=0, has_side_effects=True, vmem_limit_bytes=mib(63)),
        name="layer0",
    )(*args)


def adamw(w, m, v, g):
    m = 0.9 * m + 0.1 * g
    v = 0.95 * v + 0.05 * g * g
    step = m * lax.rsqrt(v + 1e-8) + 0.1 * w
    return w - 0.02 * step, m, v


def optimizer_kernel(count, take_ref, down_g_ref, squares_ref, wg_ref, wu_ref, wd_ref, mg_ref, mu_ref, md_ref, vg_ref, vu_ref, vd_ref,
                     send_ref, down_ref, mg_out, mu_out, md_out, vg_out, vu_out, vd_out, near, down_w, takes, g6, sends, sems):
    coords, core = place()
    x, y, z = coords
    copies = []
    for which, ref in enumerate((wg_ref, wu_ref)):
        copies.append(pltpu.make_async_copy(ref.at[:, pl.ds((RING * x + y) * ROWS, ROWS)], near.at[which], sems.at[which]))
    copies.append(pltpu.make_async_copy(wd_ref.at[:, pl.ds(number(coords, core) * ROWS, ROWS)], down_w, sems.at[DOWN]))
    begin(copies)
    squares = jnp.sum(jnp.sum(squares_ref[:], axis=0, keepdims=True), axis=1, keepdims=True)
    factor = jnp.minimum(1.0, 0.5 * lax.rsqrt(squares / count + 1e-30))
    takes[:] = take_ref[:].astype(F32)
    sends[:] = jnp.zeros_like(sends)
    end(copies)

    rows = lax.broadcasted_iota(jnp.int32, (GROUP, ROWS), 0)
    among = lax.broadcasted_iota(jnp.int32, (GROUP, ROWS), 1)
    sel = ((among == OWN * (CORES * z + core) + rows) & (rows < OWN)).astype(F32).astype(BF16)
    places = [(k, c, zz) for k in range(PARTS) for c in range(CORES) for zz in range(RING)]
    moments = ((mg_ref, vg_ref, mg_out, vg_out), (mu_ref, vu_ref, mu_out, vu_out))
    for layer in PAIR:
        for which in (GATE, UP):
            for half in PAIR:
                for n, (k, c, zz) in enumerate(places):
                    row = packed_row(layer, which, k)
                    g6[:, lanes(half * len(places) + n)] = takes[CORES * zz + c, pl.ds(row, OWN), lanes(half)]
            w = nn(sel, near[which, layer])[:OWN]
            m_in, v_in, m_out, v_out = moments[which]
            w, m_out[:, layer, :], v_out[:, layer, :] = adamw(w, m_in[:, layer, :], v_in[:, layer, :], g6[:] * factor)
            for n, (k, c, zz) in enumerate(places):
                sends[CORES * zz + c, pl.ds(packed_row(layer, which, k), OWN), :] = w[:, n * LANES : (n + 1) * LANES]
    send_ref[:] = sends[:].astype(BF16)
    for layer in PAIR:
        w, md_out[layer], vd_out[layer] = adamw(down_w[layer].astype(F32), md_ref[layer], vd_ref[layer], down_g_ref[layer] * factor)
        down_ref[layer] = w.astype(BF16)


def optimizer(sums, weights, m, v):
    shapes = shaped(F32, *(t.shape for t in m))
    packed = (GROUP, PACKED, LANES)
    return pl.pallas_call(
        functools.partial(optimizer_kernel, sum(w.size for w in weights)),
        out_shape=(*shaped(BF16, packed, (LAYERS, ROWS, D)), *shapes, *shapes),
        in_specs=[VMEM] * 3 + [ANY] * 3 + [VMEM] * 6,
        out_specs=(VMEM,) * 8,
        scratch_shapes=[
            *slots(BF16, (LAYERS, ROWS, FF), (ROWS, D)),
            pltpu.VMEM(packed, F32),
            pltpu.VMEM((OWN, FF), F32),
            pltpu.VMEM(packed, F32),
            DMA((PARTS,)),
        ],
        compiler_params=PARAMS(vmem_limit_bytes=mib(62)),
        name="optimizer",
    )(*sums, *weights, *m, *v)


def turned(moments):
    gate, up, down = moments
    return [gate.swapaxes(0, 1), up.swapaxes(0, 1), down]


def terms(x, dy, weights):
    by_gate, by_up, act0, h, scale, a0t, a1, a1t = forward(x, *weights)
    grad1, _act1, dg, du = layer1(a1, a1t, dy, *weights)
    return (grad1, *layer0(a0t, h, scale, dy, *weights, by_gate, by_up, act0, dg, du, grad1))


def local_step(x, dy, *arrays):
    weights, m, v = (arrays[i : i + PARTS] for i in range(0, len(arrays), PARTS))
    sums = terms(x[0], dy[0], weights)[-3:]
    send, down, *new = optimizer(sums, weights, turned(m), turned(v))
    spaces = (pltpu.VMEM, pltpu.VMEM, pltpu.VMEM, pltpu.HBM)
    gathered = all_gather(send, down)
    new_weights = put(*(pltpu.with_memory_space_constraint(w, space) for w, space in zip(gathered, spaces, strict=True)))
    return (*(n.reshape(w.shape) for n, w in zip(new_weights, weights, strict=True)), *turned(new[:PARTS]), *turned(new[PARTS:]))


def solution(mesh):
    moments = P(None, "dp", None)
    whole, mine = P(), P("dp")
    return jax.shard_map(
        local_step,
        mesh=mesh,
        in_specs=(mine, mine, whole, whole, whole, *(moments,) * 6),
        out_specs=(whole, whole, whole, *(moments,) * 6),
        check_vma=False,
    )
```

```python
import functools

import jax
import jax.numpy as jnp
from jax import lax
from jax.experimental import pallas as pl
from jax.experimental.pallas import tpu as pltpu
from jax.sharding import PartitionSpec as P

F32, BF16 = jnp.float32, jnp.bfloat16
MESH = pl.DeviceIdType.MESH
ALL = slice(None)
VMEM = pl.BlockSpec(memory_space=pltpu.VMEM)
ANY = pl.BlockSpec(memory_space=pl.ANY)
PARAMS = pltpu.CompilerParams
DMA = pltpu.SemaphoreType.DMA
SIGNALS = pltpu.SemaphoreType.REGULAR

RING, CORES, LAYERS = 4, 2, 2
TORUS = (RING, RING, RING)
AXES = range(len(TORUS))
PARTS = len(TORUS)
PAIR = range(2)
GROUP = RING * CORES
PLANE = RING * RING
OWN = 6
ROWS = OWN * GROUP
HALF = 128
LANES = 2 * HALF
T, D, FF = 1024, 768, 6144
NB = 512
N_J = FF // NB
STRIP = 256


def mib(n):
    return n << 20


def begin(copies):
    for c in copies:
        c.start()


def end(copies):
    for c in copies:
        c.wait()


def received(copies):
    for c in copies:
        c.wait_recv()


def sent(copies):
    for c in copies:
        c.wait_send()


def loop(n, first=0):
    def run(body):
        lax.fori_loop(first, n, lambda i, _: body(i), None)

    return run


def slot(i):
    return i % len(PAIR)


def columns(j, n=NB):
    return pl.ds(pl.multiple_of(j * n, n), n)


def lanes(q, n=HALF):
    return pl.ds(q * n, n)


def around(q):
    return q % RING


def place():
    p = lax.axis_index("dp")
    q = p // CORES
    return (q // PLANE, around(q // RING), around(q)), p % CORES


def number(coords, core):
    x, y, z = coords
    return ((x * RING + y) * RING + z) * CORES + core


def device(coords, core):
    return {"dp": number(coords, core)}


def moved(coords, axis, by):
    return tuple(around(q + by) if a == axis else q for a, q in enumerate(coords))


def signal(sem, where):
    pl.semaphore_signal(sem, inc=1, device_id=where, device_id_type=MESH)


def remote(src, dst, send, recv, where):
    return pltpu.make_async_remote_copy(src_ref=src, dst_ref=dst, send_sem=send, recv_sem=recv, device_id=where, device_id_type=MESH)


def group_peers(coords, core):
    x, y, z = coords
    return [((x, y, around(z + dz)), (core + dc) % CORES) for dz in range(RING) for dc in range(CORES) if dz or dc]


def plane_peers(coords, core):
    x, y, z = coords
    return [((around(x + dx), around(y + dy), z), core) for dx in range(RING) for dy in range(RING) if dx or dy]


def enter(coords, core):
    barrier = pltpu.get_barrier_semaphore()
    peers = group_peers(coords, core) + plane_peers(coords, core)
    for where, c in peers:
        signal(barrier, device(where, c))
    pl.semaphore_wait(barrier, len(peers))


GATE, UP, DOWN, WIDE = range(4)
ORDER = [(1, which, half) for half in PAIR for which in (GATE, UP)]
ORDER += [(layer, DOWN, half) for layer in (1, 0) for half in PAIR]
ORDER += [(0, which, half) for half in PAIR for which in (GATE, UP)]
UNITS = len(ORDER)
UNIT = {what: u for u, what in enumerate(ORDER)}
WIDE1, DOWN1, DOWN0, WIDE0 = UNIT[1, GATE, 0], UNIT[1, DOWN, 0], UNIT[0, DOWN, 0], UNIT[0, GATE, 0]
EACH = UNITS // LAYERS
AHEAD = len(PAIR)
SIDES = ((0, 1), (1, -1))
REACH = (*SIDES, (2, 2))
PASSED, DIRECT = 1, 0
CELL = (ROWS, HALF)


def pair_of(half):
    return pl.ds(2 * half, 2)


class Ring:
    def __init__(self, k, stage, coords, core, bufs, ss, rs, credit):
        self.axes = axes_left(k, stage)
        self.axis, self.cut = (k + stage) % PARTS, (k - 1) % PARTS
        self.last = self.axis == self.cut
        self.coords, self.core = coords, core
        self.data, self.ra, *self.rb = bufs
        self.ss, self.rs, self.credit = ss, rs, credit
        self.i = coords[self.axis]

    def to(self, by):
        return device(moved(self.coords, self.axis, by), self.core)

    def index(self, by, half):
        place = around(self.i + by)
        return (*(place if a == self.axis else pair_of(half) if a == self.cut else ALL for a in self.axes), ALL, ALL)

    def out(self, half):
        return (*(pair_of(half) if a == self.cut else ALL for a in self.axes if a != self.axis), ALL, ALL)

    def copy(self, n, src, dst, by):
        return remote(src, dst, self.ss.at[n], self.rs.at[n], self.to(by))

    def firsts(self):
        if self.last:
            return {n: self.copy(n, self.data.at[self.index(by, 0)], self.ra.at[n], by) for n, by in REACH}
        out = {}
        for side, by in SIDES:
            for which, step, half in ((PASSED, by + by, 1 - side), (DIRECT, by, side)):
                out[side, which] = self.copy(len(out), self.data.at[self.index(step, half)], self.ra.at[side, which], by)
        return out

    def seconds(self):
        return [self.copy(len(SIDES) * len(PAIR) + side, self.ra.at[side, PASSED], self.rb[0].at[side], by) for side, by in SIDES]

    def peers(self):
        return REACH if self.last else SIDES

    def start(self, again):
        @pl.when(again)
        def _():
            for n, _by in self.peers():
                pl.semaphore_wait(self.credit.at[n], 1)

        begin(self.firsts().values())

    def middle(self):
        copies = self.firsts()
        for side, by in SIDES:
            copies[side, PASSED].wait_recv()
            here = self.data[self.index(by, 1 - side)].astype(F32)
            self.ra[side, PASSED] = (here + self.ra[side, PASSED].astype(F32)).astype(BF16)
        begin(self.seconds())

    def finish(self, store, more):
        copies = self.firsts()
        passed = [] if self.last else self.seconds()
        if self.last:
            received(copies.values())
            store((ALL, ALL), sum(self.ra[n].astype(F32) for n, _by in REACH) + self.data[self.index(0, 0)].astype(F32))
        else:
            received([copies[side, DIRECT] for side, _by in SIDES])
            received(passed)
            for half in PAIR:
                here = self.data[self.index(0, half)].astype(F32)
                store(self.out(half), here + self.ra[half, DIRECT].astype(F32) + self.rb[0][1 - half].astype(F32))
        sent([*copies.values(), *passed])

        @pl.when(more)
        def _():
            for n, by in self.peers():
                signal(self.credit.at[n], self.to(-by))


def axes_left(k, stage):
    done = [(k + s) % PARTS for s in range(stage)]
    return [a for a in AXES if a not in done]


class Scatter:
    def __init__(self, grads, bufs, sems):
        self.grads = grads
        self.coords, self.core = place()
        self.partner = device(self.coords, 1 - self.core)
        self.d1, self.r0, self.stages, self.blocks, self.squares = bufs
        self.load_sem, self.s_send, self.s_recv, self.ssem, self.rsem, self.credit, self.s_credit = sems

    def load(self, u, k, layer=0):
        src = self.grads[layer].at[u % EACH, k, self.core]
        return pltpu.make_async_copy(src, self.d1.at[slot(u), k], self.load_sem.at[slot(u), k])

    def swap(self, u, k, layer=0):
        s = slot(u)
        src = self.grads[layer].at[u % EACH, k, 1 - self.core]
        return remote(src, self.r0.at[s, k], self.s_send.at[s, k], self.s_recv.at[s, k], self.partner)

    def rings(self, u, stage):
        s = slot(u)
        return [
            Ring(k, stage, self.coords, self.core, [b.at[s] for b in self.stages[stage][k]], self.ssem.at[s, k, stage], self.rsem.at[s, k, stage],
                 self.credit.at[k, stage])
            for k in range(PARTS)
        ]

    def start(self, u, copy):
        for layer, its in ((1, u < EACH), (0, u >= EACH)):

            @pl.when(its)
            def _(layer=layer):
                begin([copy(u, k, layer) for k in range(PARTS)])

    def start_swap(self, u):
        @pl.when(u >= AHEAD)
        def _():
            pl.semaphore_wait(self.s_credit, 1)

        self.start(u, self.swap)

    def start_load(self, u):
        self.start(u, self.load)

    def add(self, u):
        for k in range(PARTS):
            self.load(u, k).wait()
            self.swap(u, k).wait_recv()
            d1, r0 = self.d1.at[slot(u), k], self.r0.at[slot(u), k]

            @loop(PLANE)
            def _(n, d1=d1, r0=r0):
                at = (n // RING, around(n))
                d1[at] = (d1[at].astype(F32) + r0[at].astype(F32)).astype(BF16)

        sent([self.swap(u, k) for k in range(PARTS)])

        @pl.when(u + AHEAD < UNITS)
        def _():
            signal(self.s_credit, self.partner)

        for ring in self.rings(u, 0):
            ring.start(u >= AHEAD)

    def at_stages(self, i, stages, step):
        for stage in reversed(stages):
            u = i - stage

            @pl.when((u >= 0) & (u < UNITS))
            def _(u=u, stage=stage):
                step(u, stage)

    def middles(self, i):
        def step(u, stage):
            for ring in self.rings(u, stage):
                ring.middle()

        self.at_stages(i, AXES[:-1], step)

    def finishes(self, i):
        def step(u, stage):
            rings = self.rings(u, stage)
            for k, ring in enumerate(rings):
                ring.finish(self.into(u, k, ring, stage), u + AHEAD < UNITS)
            if not rings[0].last:
                for ring in self.rings(u, stage + 1):
                    ring.start(u >= AHEAD)

        self.at_stages(i, AXES, step)

    def into(self, u, k, ring, stage):
        def store(at, value):
            value = value.astype(BF16)
            if not ring.last:
                self.stages[stage + 1][k][0][(slot(u),) + at] = value
                return
            self.blocks[(u, k) + at] = value
            value = value.astype(F32)
            self.squares[:] += jnp.sum((value * value).reshape(-1, *self.squares.shape), axis=0)

        return store


PACKED = 80


def packed_row(layer, which, k):
    return OWN * ((layer * len(PAIR) + which) * PARTS + k)


def scatter_scratch():
    two = (len(PAIR),)
    out = [pltpu.VMEM((*two, PARTS, *TORUS, *CELL), BF16)] * len(PAIR)
    for stage in AXES:
        for k in range(PARTS):
            left = [len(PAIR) if a == (k - 1) % PARTS else RING for a in axes_left(k, stage + 1)]
            if left:
                out.append(pltpu.VMEM((*two, *(RING for _ in left), *CELL), BF16))
                out.append(pltpu.VMEM((*two, *two, *two, *left, *CELL), BF16))
                out.append(pltpu.VMEM((*two, *two, *left, *CELL), BF16))
            else:
                out.append(pltpu.VMEM((*two, len(REACH), *CELL), BF16))
    each = (*two, PARTS)
    out += [pltpu.VMEM((UNITS, PARTS, *CELL), BF16), pltpu.VMEM((8, HALF), F32)]
    out += [DMA(each)] * PARTS + [DMA((*each, PARTS, 6))] * len(PAIR) + [SIGNALS((PARTS, PARTS, len(REACH))), SIGNALS]
    out += [pltpu.VMEM((PACKED, LANES), F32), pltpu.VMEM((GROUP, PACKED, LANES), BF16), pltpu.VMEM((GROUP, PACKED, LANES), BF16)]
    out += [pltpu.VMEM((PLANE, *two, 8, HALF), F32)]
    return out + [DMA((GROUP,))] * 4 + [DMA((PLANE,))] * 2


def scatter_of(grads, scratch):
    scratch = iter(scratch)
    d1, r0 = next(scratch), next(scratch)
    stages = []
    data = [d1.at[:, k] for k in range(PARTS)]
    for stage in AXES:
        row, after = [], []
        for k in range(PARTS):
            own = [data[k]]
            if axes_left(k, stage + 1):
                after.append(next(scratch))
                own.append(next(scratch))
            row.append((*own, next(scratch)))
        stages.append(row)
        data = after
    blocks, squares, *rest = scratch
    return Scatter(grads, (d1, r0, stages, blocks, squares), rest[:7]), rest[7:]


def last_swap(sc, out_ref, own_ref, ss_ref, stage, pack, take, sq, t_send, t_recv, q_send, q_recv, q2_send, q2_recv):
    coords, core = sc.coords, sc.core
    x, y, z = coords
    me = CORES * z + core
    first, second = (sq.at[:, i] for i in PAIR)
    peers = list(enumerate(group_peers(coords, core)))
    first[me] = sc.squares[:]
    squares = [remote(first.at[me], first.at[me], q_send.at[n], q_recv.at[n], device(where, c)) for n, (where, c) in peers]
    takes = [remote(pack.at[CORES * where[-1] + c], take.at[me], t_send.at[n], t_recv.at[n], device(where, c)) for n, (where, c) in peers]
    begin(squares)
    stage[:] = jnp.zeros_like(stage)
    for j in range(GROUP):
        for u, (layer, which, half) in enumerate(ORDER):
            for k in range(PARTS):
                if which != DOWN:
                    stage[pl.ds(packed_row(layer, which, k), OWN), lanes(half)] = sc.blocks[u, k].astype(F32)[OWN * j : OWN * j + OWN]
        pack[j] = stage[:].astype(BF16)
    begin(takes)
    for u, (layer, which, half) in enumerate(ORDER):
        for k in range(PARTS):
            if which == DOWN:
                own_ref[layer, :, lanes(half * PARTS + k)] = sc.blocks[u, k].astype(F32)
    take[me] = pack[me]
    received(squares)
    total = sum(first[j] for j in range(GROUP))
    sent(squares)
    mine = RING * x + y
    second[mine] = total
    squares = [
        remote(second.at[mine], second.at[mine], q2_send.at[n], q2_recv.at[n], device(where, c)) for n, (where, c) in enumerate(plane_peers(coords, core))
    ]
    begin(squares)
    end(takes)
    out_ref[:] = take[:]
    end(squares)
    ss_ref[:] = sum(second[j] for j in range(PLANE))


def gather_kernel(rows_ref, down_ref, wide_out, down0_out, down1_out, last_out, take, stage, t_send, t_recv, own_sem, send, recv, c_send, c_recv):
    coords, core = place()
    x, y, z = coords
    me = CORES * z + core
    partner = device(coords, 1 - core)
    enter(coords, core)
    swaps = []
    for n, (where, c) in enumerate(group_peers(coords, core)):
        swaps.append(remote(rows_ref.at[CORES * where[-1] + c], take.at[me], t_send.at[n], t_recv.at[n], device(where, c)))
    begin(swaps)
    here = (*coords, core)
    own = pltpu.make_async_copy(down_ref.at[1, :, lanes(PARTS - 1, LANES)], last_out.at[here], own_sem)
    own.start()
    down0_out[here] = down_ref[0]
    down1_out[here] = down_ref[1, :, pl.ds(0, D - LANES)]

    def piece(which, k, layer, spot):
        at = tuple(ALL if q is None else q for q in spot)
        if which == DOWN:
            if layer and k == PARTS - 1:
                return last_out.at[(*at, core)]
            return (down0_out, down1_out)[layer].at[(*at, core, ALL, lanes(k, LANES))]
        matrix = ALL if which == WIDE else which
        base = (k * GROUP + core * RING) * LANES
        many = RING if spot[-1] is None else 1
        if many == 1:
            base += spot[-1] * LANES
        return wide_out.at[(layer, matrix, *at[:-1], ALL, pl.ds(pl.multiple_of(base, many * LANES), many * LANES))]

    def unpack():
        take[me] = rows_ref[me]
        received(swaps)
        for j in range(GROUP):
            rows = take[j].astype(F32)
            for q in range(len(stage)):
                stage[q, pl.ds(OWN * j, OWN), :] = rows[OWN * q : OWN * q + OWN]
        for layer in PAIR:
            for which in (GATE, UP):
                for k in range(PARTS):
                    at = pl.multiple_of((GROUP * k + RING * core + z) * LANES, LANES)
                    wide_out[layer, which, x, y, :, pl.ds(at, LANES)] = stage[packed_row(layer, which, k) // OWN].astype(BF16)
        sent(swaps)

    def spot(k, turn, by):
        out = []
        for a in AXES:
            its = (k - 1 - a) % PARTS
            out.append(None if its < turn else around(coords[a] + by) if its == turn else coords[a])
        return out

    shares = []

    def share(which, k, layer, turn, by, n):
        ref = piece(which, k, layer, spot(k, turn, by))
        shares.append(remote(ref, ref, c_send.at[k, turn, which % PARTS, n], c_recv.at[k, turn, which % PARTS, n], partner))
        shares[-1].start()

    class Turn:
        def __init__(self, matrices, turn):
            self.turn = turn
            self.all = [(which, k, side, by) for which in matrices for k in range(PARTS) for side, by in SIDES]
            self.first = [self.copy(which, k, by, side, side, 0) for which, k, side, by in self.all]
            self.other = [self.copy(which, k, by, 2 + side, 1 - side, 0) for which, k, side, by in self.all]
            self.far = [self.copy(which, k, by, 4 + side, side, -by) for which, k, side, by in self.all]

        def copy(self, which, k, by, n, layer, start):
            ref = piece(which, k, layer, spot(k, self.turn, start))
            sems = send.at[k, self.turn, which % PARTS, n], recv.at[k, self.turn, which % PARTS, n]
            return remote(ref, ref, *sems, device(moved(coords, (k - 1 - self.turn) % PARTS, by), core))

        def start(self):
            begin(self.first)
            begin(self.other)
            if self.turn == 0:
                for which, k, side, by in self.all:
                    share(which, k, side, self.turn, 0, side)

        def near(self):
            for n, (which, k, side, by) in enumerate(self.all):
                self.first[n].wait_recv()
                self.far[n].start()
                share(which, k, side, self.turn, -by, 2 + side)
            for n, (which, k, side, by) in enumerate(self.all):
                self.other[n].wait_recv()
                share(which, k, 1 - side, self.turn, -by, 4 + side)

        def done(self):
            for n, (which, k, side, by) in enumerate(self.all):
                self.far[n].wait_recv()
                share(which, k, side, self.turn, 2, 6 + side)
            sent(self.first + self.other + self.far)

    streams = [[Turn(matrices, turn) for matrices in ((DOWN,), (WIDE,) if turn < AXES[-1] else (GATE, UP))] for turn in AXES]
    own.wait()
    for downs, wides in streams:
        if downs.turn == 0:
            downs.start()
            unpack()
            wides.start()
        downs.near()
        wides.near()
        for stream, now in enumerate((downs, wides)):
            now.done()
            if now.turn + 1 < len(streams):
                streams[now.turn + 1][stream].start()
    end(shares)


def all_gather(rows, down):
    owners = (*TORUS, CORES, ROWS)
    return pl.pallas_call(
        gather_kernel,
        out_shape=(
            pltpu.VMEM((LAYERS, len(PAIR), RING, RING, ROWS, FF), BF16),
            pltpu.VMEM((*owners, D), BF16),
            pltpu.VMEM((*owners, D - LANES), BF16),
            jax.ShapeDtypeStruct((*owners, LANES), BF16),
        ),
        in_specs=[VMEM] * 2,
        out_specs=(VMEM, VMEM, VMEM, ANY),
        scratch_shapes=[
            pltpu.VMEM(rows.shape, BF16),
            pltpu.VMEM((LAYERS * len(PAIR) * PARTS, ROWS, LANES), F32),
            *[DMA((GROUP,))] * 2,
            DMA,
            *[DMA((PARTS, PARTS, PARTS, 6))] * 2,
            *[DMA((PARTS, PARTS, PARTS, 8))] * 2,
        ],
        compiler_params=PARAMS(collective_id=1, has_side_effects=True, vmem_limit_bytes=mib(4)),
        name="all_gather",
    )(rows, down)


def put_kernel(wide_ref, down0_ref, down1_ref, last_ref, gate_out, up_out, down_out, bounce, sems):
    def into(ref, start, n):
        return ref.at[(1, *(ALL for _ in bounce.shape[:-1]), pl.ds(start, n))]

    pairs = [(wide_ref.at[layer, which], out.at[layer]) for layer in PAIR for which, out in ((GATE, gate_out), (UP, up_out))]
    pairs += [(down0_ref, down_out.at[0]), (down1_ref, into(down_out, 0, D - LANES))]
    pairs += [(last_ref, bounce), (bounce, into(down_out, D - LANES, LANES))]
    *copies, come, go = [pltpu.make_async_copy(src, dst, sems.at[n]) for n, (src, dst) in enumerate(pairs)]
    come.start()
    begin(copies)
    come.wait()
    go.start()
    end(copies)
    go.wait()


def put(wide, down0, down1, last):
    wide_shape = jax.ShapeDtypeStruct((LAYERS, *wide.shape[2:]), BF16)
    return pl.pallas_call(
        put_kernel,
        out_shape=(wide_shape, wide_shape, jax.ShapeDtypeStruct((LAYERS, *down0.shape), BF16)),
        in_specs=[VMEM, VMEM, VMEM, ANY],
        out_specs=(ANY, ANY, ANY),
        scratch_shapes=[pltpu.VMEM(last.shape, BF16), DMA((GROUP,))],
        compiler_params=PARAMS(vmem_limit_bytes=mib(4)),
        name="put",
    )(wide, down0, down1, last)


def nn(a, b):
    return jnp.dot(a, b, preferred_element_type=F32)


def nt(a, b):
    return lax.dot_general(a, b, (((1,), (1,)), ((), ())), preferred_element_type=F32)


def tn(a, b):
    return lax.dot_general(a, b, (((0,), (0,)), ((), ())), preferred_element_type=F32)


def rms(wide):
    return lax.rsqrt(jnp.mean(wide * wide, -1, keepdims=True) + 1e-6)


def sigmoid(g):
    return 0.5 * jnp.tanh(0.5 * g) + 0.5


def strips():
    return [pl.ds(r, STRIP) for r in range(0, T, STRIP)]


def factors(g, u):
    sig = sigmoid(g)
    silu = g * sig
    return u * (sig + silu * (1 - sig)), silu, (silu * u).astype(BF16)


def forward_part(x_ref, wg_ref, wu_ref, wd_ref, g_ref, u_ref, act_ref, h_ref, scale_ref, a0t_ref, a1_ref, a1t_ref,
                 a0, wg, wu, wd, gate, up, act, w_sem, d_sem, g_sem, a_sem, meanwhile):
    def weights(j):
        s = slot(j)
        return [pltpu.make_async_copy(ref.at[0, :, columns(j)], buf.at[s], w_sem.at[n, s]) for n, (ref, buf) in enumerate(((wg_ref, wg), (wu_ref, wu)))]

    def downs(n):
        return [pltpu.make_async_copy(wd_ref.at[0, :, columns(n, LANES)], wd.at[slot(n)], d_sem.at[slot(n)])]

    def stores(j):
        s = slot(j)
        out = [pltpu.make_async_copy(buf.at[s], ref.at[:, columns(j)], g_sem.at[n, s]) for n, (ref, buf) in enumerate(((g_ref, gate), (u_ref, up)))]
        return out + [pltpu.make_async_copy(act.at[:, columns(j)], act_ref.at[:, columns(j)], a_sem.at[s])]

    def norm(from_ref, to_ref, turned_ref):
        @loop(T // STRIP)
        def _(i):
            rows = columns(i, STRIP)
            wide = from_ref[rows, :].astype(F32)
            scale = rms(wide)
            scale_ref[rows, :] = jnp.broadcast_to(scale, (STRIP, HALF))
            a = (wide * scale).astype(BF16)
            to_ref[rows, :] = a
            turned_ref[:, rows] = a.T

    begin(weights(0))
    begin(downs(0))
    norm(x_ref, a0, a0t_ref)

    @loop(N_J)
    def _(j):
        s = slot(j)
        end(weights(j))

        @pl.when(j >= AHEAD)
        def _():
            end(stores(j - AHEAD))

        @pl.when(j + 1 < N_J)
        def _():
            begin(weights(j + 1))

        for rows in strips():
            gate[s, rows, :], up[s, rows, :], act[rows, columns(j)] = factors(nn(a0[rows, :], wg[s]), nn(a0[rows, :], wu[s]))
        begin(stores(j))

    @loop(D // LANES)
    def _(n):
        end(downs(n))

        @pl.when(n + 1 < D // LANES)
        def _():
            begin(downs(n + 1))

        for r in range(0, T, NB):
            rows = pl.ds(r, NB)
            y = nn(act[rows, :], wd[slot(n)]).astype(BF16)
            h_ref[rows, columns(n, LANES)] = x_ref[rows, columns(n, LANES)] + y

    meanwhile()
    norm(h_ref, a1_ref, a1t_ref)
    for j in PAIR:
        end(stores(N_J - AHEAD + j))


def shaped(dtype, *shapes):
    return tuple(jax.ShapeDtypeStruct(s, dtype) for s in shapes)


def slots(dtype, *shapes):
    return [pltpu.VMEM((len(PAIR), *s), dtype) for s in shapes]


def both_of(a, b):
    return tuple(enumerate(zip(a, b, strict=True)))


def tiles_of(layer, wide_refs, down_ref, wide_bufs, down_buf, sem):
    def copies(j):
        s = slot(j)
        wide = [pltpu.make_async_copy(ref.at[layer, :, columns(j)], buf.at[s], sem.at[n, s]) for n, (ref, buf) in both_of(wide_refs, wide_bufs)]
        return wide + [pltpu.make_async_copy(down_ref.at[layer, columns(j)], down_buf.at[s], sem.at[DOWN, s])]

    return copies


def wide_outs(grad_ref, first, bufs, sem):
    def copies(j):
        s, q = slot(j), j % EACH
        u = first + len(PAIR) * (j // EACH)
        return [pltpu.make_async_copy(buf.at[s], grad_ref.at[u + n, q // CORES, q % CORES], sem.at[n, s]) for n, buf in enumerate(bufs)]

    return copies


def wide_terms(at_ref, terms, bufs, s):
    for n, dst in enumerate(bufs):
        w = nn(at_ref[:], terms[s, n]).astype(BF16)
        for z in range(RING):
            dst[s, :, :, z] = w[:, z * HALF : (z + 1) * HALF].reshape(RING, RING, ROWS, HALF)


TILES = FF // D


def down_parts(grad_ref, first, act_hbm, d_ref, act, out, a_sem, d_sem):
    def comes(t):
        return [pltpu.make_async_copy(act_hbm.at[:, columns(t, D)], act.at[slot(t)], a_sem.at[slot(t)])]

    def goes(t):
        s = slot(t)
        x, y = t // len(PAIR), pair_of(s)
        return [pltpu.make_async_copy(out.at[s, h], grad_ref.at[first + h, :, :, x, y], d_sem.at[h, s]) for h in PAIR]

    def step(t):
        s = slot(t)
        end(comes(t))

        @pl.when(t >= AHEAD)
        def _():
            end(goes(t - AHEAD))

        @pl.when(t + 1 < TILES)
        def _():
            begin(comes(t + 1))

        w = tn(act[s], d_ref[:]).astype(BF16).reshape(len(PAIR), RING, CORES, ROWS, D)
        for h in PAIR:
            for k in range(PARTS):
                at = (h * PARTS + k) * HALF
                for c in range(CORES):
                    out[s, h, k, c] = w[:, :, c, :, at : at + HALF]
        begin(goes(t))

    def finish():
        for t in PAIR:
            end(goes(TILES - AHEAD + t))

    return comes, step, finish


def layer1_kernel(x_ref, dy_ref, wg_ref, wu_ref, wd_ref, g_ref, u_ref, act0_ref, h_ref, scale_ref, a0t_ref, grad_ref, act1_ref, dg_ref, du_ref,
                  a0, a1_ref, a1t_ref, wide_down, gate, up, act0, f_sem, g_sem, h_sem,
                  wg, wu, wd, act, terms, out_g, out_u, out_d, w_sem, o_sem, d_sem, a_sem, t_sem):
    weights = tiles_of(1, (wg_ref, wu_ref), wd_ref, (wg, wu), wd, w_sem)
    outs = wide_outs(grad_ref, 0, (out_g, out_u), o_sem)

    def back(j):
        s = slot(j)
        pairs = both_of((terms.at[s, GATE], terms.at[s, UP], act.at[s, :, pl.ds(0, NB)]), (dg_ref, du_ref, act1_ref))
        return [pltpu.make_async_copy(src, dst.at[:, columns(j)], t_sem.at[n, s]) for n, (src, dst) in pairs]

    forward_part(x_ref, wg_ref, wu_ref, wd_ref, g_ref, u_ref, act0_ref, h_ref, scale_ref, a0t_ref, a1_ref, a1t_ref,
                 a0, wg, wu, wide_down, gate, up, act0, w_sem, f_sem, g_sem, h_sem, lambda: begin(weights(0)))

    @loop(N_J)
    def _(j):
        s = slot(j)
        end(weights(j))

        @pl.when(j >= AHEAD)
        def _():
            end(back(j - AHEAD))
            end(outs(j - AHEAD))

        @pl.when(j + 1 < N_J)
        def _():
            begin(weights(j + 1))

        for rows in strips():
            by_gate, by_up, a = factors(nn(a1_ref[rows, :], wg[s]), nn(a1_ref[rows, :], wu[s]))
            d = nt(dy_ref[rows, :], wd[s]).astype(BF16).astype(F32)
            act[s, rows, pl.ds(0, NB)] = a
            terms[s, GATE, rows, :] = (d * by_gate).astype(BF16)
            terms[s, UP, rows, :] = (d * by_up).astype(BF16)
        wide_terms(a1t_ref, terms, (out_g, out_u), s)
        begin(back(j))
        begin(outs(j))

    for j in PAIR:
        end(back(N_J - AHEAD + j))
        end(outs(N_J - AHEAD + j))
    comes, step, finish = down_parts(grad_ref, RING, act1_ref, dy_ref, act, out_d, a_sem, d_sem)
    begin(comes(0))
    loop(TILES)(step)
    finish()


FIRST_DOWN = N_J
FIRST_WIDE = FIRST_DOWN + TILES
LAST_STEPS = FIRST_WIDE + N_J
STEPS = LAST_STEPS + 6
MIDDLES = (4, 8, 11, 15, 21, 23, 25, 27, 30, *range(LAST_STEPS + 1, STEPS - 1))
ADDS = (2, 3, 8, 11, 14, 21, 23, 25, 28, 29, LAST_STEPS + 1, LAST_STEPS + 2)
FINISHES = (7, 10, 13, 20, 22, 24, 26, 28, *range(LAST_STEPS, STEPS))
LOADS = FINISHES[: UNITS - AHEAD]
SWAPS = (2, 3, 8, 11, 19, 21, 26, 27, LAST_STEPS - 1, LAST_STEPS)


def due(step, steps, do):
    now = functools.reduce(jnp.logical_or, [step == at for at in steps])
    n = sum((step > at).astype(jnp.int32) for at in steps)

    @pl.when(now)
    def _():
        do(n)


def layer0_kernel(a0t_hbm, h_hbm, scale_hbm, dy_hbm, wg_ref, wu_ref, wd_ref, g_ref, u_ref, act0_ref, dg_ref, du_ref, grad1_ref,
                  grad_ref, take_ref, own_ref, ss_ref,
                  a0t_ref, h_ref, scale_ref, dy_ref, i_sem,
                  wg, wu, wd, act, terms, out_g, out_u, out_d, gate, up, total, dh,
                  w_sem, o_sem, d_sem, a_sem, l_sem, t_sem, *scratch):
    sc, rest = scatter_of((grad_ref, grad1_ref), scratch)
    weights = tiles_of(0, (wg_ref, wu_ref), wd_ref, (wg, wu), wd, w_sem)
    outs = wide_outs(grad_ref, len(PAIR), (out_g, out_u), o_sem)
    comes, down_step, down_finish = down_parts(grad_ref, 0, act0_ref, dh, act, out_d, a_sem, d_sem)
    sources = both_of((dg_ref, du_ref), zip((wg_ref, wu_ref), (wg, wu), strict=True))

    def products(j):
        s = slot(j)
        return [pltpu.make_async_copy(ref.at[:, columns(j)], buf.at[s], l_sem.at[n, s]) for n, (ref, buf) in both_of((g_ref, u_ref), (gate, up))]

    def da_in(j):
        s, out = slot(j), []
        for n, (d_from, (w_from, w_to)) in sources:
            out.append(pltpu.make_async_copy(d_from.at[:, columns(j)], terms.at[s, n], t_sem.at[n, s]))
            out.append(pltpu.make_async_copy(w_from.at[1, :, columns(j)], w_to.at[s], w_sem.at[n, s]))
        return out

    def da_step(j):
        s = slot(j)
        end(da_in(j))

        @pl.when(j + 1 < N_J)
        def _():
            begin(da_in(j + 1))

        for n, (_d, (_w, w)) in sources:
            for rows in strips():
                total[n, rows, :] += nt(terms[s, n, rows, :], w[s])

    def states_step():
        @loop(T // STRIP)
        def _(i):
            rows = columns(i, STRIP)
            wide = h_ref[rows, :].astype(F32)
            scale = scale_ref[rows, pl.ds(0, 1)]
            da = sum(total[n, rows, :].astype(BF16) for n in PAIR).astype(F32)
            mean = jnp.sum(da * wide, -1, keepdims=True) * (1 / D)
            d = da * scale - wide * (mean * scale * scale * scale)
            dh[rows, :] = dy_ref[rows, :] + d.astype(BF16)

    def wide_step(j):
        s = slot(j)
        end(weights(j))
        end(products(j))

        @pl.when(j + 1 < N_J)
        def _():
            begin(weights(j + 1))
            begin(products(j + 1))

        for rows in strips():
            d = nt(dh[rows, :], wd[s]).astype(BF16).astype(F32)
            terms[s, GATE, rows, :] = (d * gate[s, rows, :]).astype(BF16)
            terms[s, UP, rows, :] = (d * up[s, rows, :]).astype(BF16)
        wide_terms(a0t_ref, terms, (out_g, out_u), s)

        @pl.when(j >= 1)
        def _():
            end(outs(j - 1))

        begin(outs(j))

    inputs = [pltpu.make_async_copy(src, dst, i_sem.at[n]) for n, (src, dst) in both_of((a0t_hbm, h_hbm, scale_hbm, dy_hbm), (a0t_ref, h_ref, scale_ref, dy_ref))]
    begin(da_in(0))
    begin(inputs)
    begin(comes(0))
    begin(products(0))
    enter(sc.coords, sc.core)
    sc.squares[:] = jnp.zeros_like(sc.squares)
    for u in range(AHEAD):
        sc.start_swap(u)
        sc.start_load(u)
    total[:] = jnp.zeros_like(total)

    @loop(STEPS)
    def _(step):
        @pl.when(step < FIRST_DOWN)
        def _():
            da_step(step)

        @pl.when(step == FIRST_DOWN - 1)
        def _():
            begin(weights(0))
            end(inputs)
            states_step()

        @pl.when((step >= FIRST_DOWN) & (step < FIRST_WIDE))
        def _():
            down_step(step - FIRST_DOWN)

        @pl.when(step == FIRST_WIDE - 1)
        def _():
            down_finish()

        @pl.when((step >= FIRST_WIDE) & (step < LAST_STEPS))
        def _():
            wide_step(step - FIRST_WIDE)

        @pl.when(step == LAST_STEPS - 1)
        def _():
            end(outs(N_J - 1))

        due(step, MIDDLES, sc.middles)
        due(step, ADDS, sc.add)
        due(step, FINISHES, sc.finishes)
        due(step, LOADS, lambda n: sc.start_load(n + AHEAD))
        due(step, SWAPS, lambda n: sc.start_swap(n + AHEAD))

    last_swap(sc, take_ref, own_ref, ss_ref, *rest)


TWO = len(PAIR)
OUT_TILE = (*TORUS, *CELL)
GRAD = (EACH, PARTS, CORES, *OUT_TILE)


def tile_buffers():
    return [
        *slots(BF16, (D, NB), (D, NB), (NB, D), (T, D), (TWO, T, NB)),
        *slots(BF16, OUT_TILE, OUT_TILE, (TWO, PARTS, CORES, TWO, RING, *CELL)),
    ]


def tile_semaphores():
    return [DMA((PARTS, TWO)), DMA((TWO, TWO)), DMA((TWO, TWO)), DMA((TWO,))]


def layer1(x, dy, *weights):
    return pl.pallas_call(
        layer1_kernel,
        out_shape=(
            *shaped(F32, (T, FF), (T, FF)),
            *shaped(BF16, (T, FF), (T, D)),
            *shaped(F32, (T, HALF)),
            *shaped(BF16, (D, T), GRAD, (T, FF), (T, FF), (T, FF)),
        ),
        in_specs=[VMEM] * 2 + [ANY] * 3,
        out_specs=(ANY,) * 3 + (VMEM,) * 3 + (ANY,) * 4,
        scratch_shapes=[
            *[pltpu.VMEM(s, BF16) for s in ((T, D), (T, D), (D, T))],
            *slots(BF16, (FF, LANES)),
            *slots(F32, (T, NB), (T, NB)),
            pltpu.VMEM((T, FF), BF16),
            DMA((TWO,)),
            DMA((TWO, TWO)),
            DMA((TWO,)),
            *tile_buffers(),
            *tile_semaphores(),
            DMA((PARTS, TWO)),
        ],
        cost_estimate=pl.CostEstimate(flops=18 * T * D * FF, bytes_accessed=mib(220), transcendentals=2 * T * FF),
        compiler_params=PARAMS(vmem_limit_bytes=mib(63)),
        name="layer1",
    )(x, dy, *weights)


def layer0(*args):
    return pl.pallas_call(
        layer0_kernel,
        out_shape=(*shaped(BF16, GRAD, (GROUP, PACKED, LANES)), *shaped(F32, (LAYERS, ROWS, D), (8, HALF))),
        in_specs=[ANY] * 13,
        out_specs=(ANY, VMEM, VMEM, VMEM),
        scratch_shapes=[
            pltpu.VMEM((D, T), BF16),
            pltpu.VMEM((T, D), BF16),
            pltpu.VMEM((T, HALF), F32),
            pltpu.VMEM((T, D), BF16),
            DMA((RING,)),
            *tile_buffers(),
            *slots(F32, (T, NB), (T, NB), (T, D)),
            pltpu.VMEM((T, D), BF16),
            *tile_semaphores(),
            DMA((TWO, TWO)),
            DMA((TWO, TWO)),
            *scatter_scratch(),
        ],
        cost_estimate=pl.CostEstimate(flops=12 * T * D * FF, bytes_accessed=mib(200), transcendentals=T * FF),
        compiler_params=PARAMS(collective_id=0, has_side_effects=True, vmem_limit_bytes=mib(63)),
        name="layer0",
    )(*args)


def adamw(w, m, v, g):
    m = 0.9 * m + 0.1 * g
    v = 0.95 * v + 0.05 * g * g
    step = m * lax.rsqrt(v + 1e-8) + 0.1 * w
    return w - 0.02 * step, m, v


def optimizer_kernel(count, take_ref, down_g_ref, squares_ref, wg_ref, wu_ref, wd_ref, mg_ref, mu_ref, md_ref, vg_ref, vu_ref, vd_ref,
                     send_ref, down_ref, mg_out, mu_out, md_out, vg_out, vu_out, vd_out, near, down_w, takes, g6, sends, sems):
    coords, core = place()
    x, y, z = coords
    copies = []
    for which, ref in enumerate((wg_ref, wu_ref)):
        copies.append(pltpu.make_async_copy(ref.at[:, pl.ds((RING * x + y) * ROWS, ROWS)], near.at[which], sems.at[which]))
    copies.append(pltpu.make_async_copy(wd_ref.at[:, pl.ds(number(coords, core) * ROWS, ROWS)], down_w, sems.at[DOWN]))
    begin(copies)
    squares = jnp.sum(jnp.sum(squares_ref[:], axis=0, keepdims=True), axis=1, keepdims=True)
    factor = jnp.minimum(1.0, 0.5 * lax.rsqrt(squares / count + 1e-30))
    takes[:] = take_ref[:].astype(F32)
    sends[:] = jnp.zeros_like(sends)
    end(copies)

    rows = lax.broadcasted_iota(jnp.int32, (GROUP, ROWS), 0)
    among = lax.broadcasted_iota(jnp.int32, (GROUP, ROWS), 1)
    sel = ((among == OWN * (CORES * z + core) + rows) & (rows < OWN)).astype(F32).astype(BF16)
    places = [(k, c, zz) for k in range(PARTS) for c in range(CORES) for zz in range(RING)]
    moments = ((mg_ref, vg_ref, mg_out, vg_out), (mu_ref, vu_ref, mu_out, vu_out))
    for layer in PAIR:
        for which in (GATE, UP):
            for half in PAIR:
                for n, (k, c, zz) in enumerate(places):
                    row = packed_row(layer, which, k)
                    g6[:, lanes(half * len(places) + n)] = takes[CORES * zz + c, pl.ds(row, OWN), lanes(half)]
            w = nn(sel, near[which, layer])[:OWN]
            m_in, v_in, m_out, v_out = moments[which]
            w, m_out[:, layer, :], v_out[:, layer, :] = adamw(w, m_in[:, layer, :], v_in[:, layer, :], g6[:] * factor)
            for n, (k, c, zz) in enumerate(places):
                sends[CORES * zz + c, pl.ds(packed_row(layer, which, k), OWN), :] = w[:, n * LANES : (n + 1) * LANES]
    send_ref[:] = sends[:].astype(BF16)
    for layer in PAIR:
        w, md_out[layer], vd_out[layer] = adamw(down_w[layer].astype(F32), md_ref[layer], vd_ref[layer], down_g_ref[layer] * factor)
        down_ref[layer] = w.astype(BF16)


def optimizer(sums, weights, m, v):
    shapes = shaped(F32, *(t.shape for t in m))
    packed = (GROUP, PACKED, LANES)
    return pl.pallas_call(
        functools.partial(optimizer_kernel, sum(w.size for w in weights)),
        out_shape=(*shaped(BF16, packed, (LAYERS, ROWS, D)), *shapes, *shapes),
        in_specs=[VMEM] * 3 + [ANY] * 3 + [VMEM] * 6,
        out_specs=(VMEM,) * 8,
        scratch_shapes=[
            *slots(BF16, (LAYERS, ROWS, FF), (ROWS, D)),
            pltpu.VMEM(packed, F32),
            pltpu.VMEM((OWN, FF), F32),
            pltpu.VMEM(packed, F32),
            DMA((PARTS,)),
        ],
        compiler_params=PARAMS(vmem_limit_bytes=mib(62)),
        name="optimizer",
    )(*sums, *weights, *m, *v)


def turned(moments):
    gate, up, down = moments
    return [gate.swapaxes(0, 1), up.swapaxes(0, 1), down]


def terms(x, dy, weights):
    by_gate, by_up, act0, h, scale, a0t, grad1, _act1, dg, du = layer1(x, dy, *weights)
    return (grad1, *layer0(a0t, h, scale, dy, *weights, by_gate, by_up, act0, dg, du, grad1))


def local_step(x, dy, *arrays):
    weights, m, v = (arrays[i : i + PARTS] for i in range(0, len(arrays), PARTS))
    sums = terms(x[0], dy[0], weights)[-3:]
    send, down, *new = optimizer(sums, weights, turned(m), turned(v))
    spaces = (pltpu.VMEM, pltpu.VMEM, pltpu.VMEM, pltpu.HBM)
    gathered = all_gather(send, down)
    new_weights = put(*(pltpu.with_memory_space_constraint(w, space) for w, space in zip(gathered, spaces, strict=True)))
    return (*(n.reshape(w.shape) for n, w in zip(new_weights, weights, strict=True)), *turned(new[:PARTS]), *turned(new[PARTS:]))


def solution(mesh):
    moments = P(None, "dp", None)
    whole, mine = P(), P("dp")
    return jax.shard_map(
        local_step,
        mesh=mesh,
        in_specs=(mine, mine, whole, whole, whole, *(moments,) * 6),
        out_specs=(whole, whole, whole, *(moments,) * 6),
        check_vma=False,
    )
```
